8 devices in a mesh: batch: 1 (over z), row: 2 (over y), col: 4 (over x, core).
Axes of the slice: x: 2, y: 2, z: 1, core: 2. Of those that a mesh axis runs over, the one named last changes fastest.
Arguments:
- l_mat: bfloat16 [8192, 8192], P(('batch', 'row'), 'col')
- b_mat: bfloat16 [8192, 16384], P(('batch', 'row'), 'col')
Outputs:
- output: bfloat16 [8192, 16384], P(('batch', 'row'), 'col')
All inputs are finite; a program needn't handle non-finite values.
Results may differ from the reference program's by a relative error of at most 0.001.
Values are sent between devices in bfloat16 or wider.
A program may use at most 1 GiB of HBM per device.

```python
import jax
import jax.numpy as jnp

N = 8192
M = 16384


def setup_inputs(seed: int = 0, part: int = 0) -> dict:
    base_key = jax.random.fold_in(jax.random.key(seed), part)
    key_l, key_b = jax.random.split(base_key)
    row_scale = 1.0 / jnp.sqrt(jnp.arange(N, dtype=jnp.float32) + 1.0)
    l_full = jax.random.normal(key_l, (N, N), jnp.float32)
    l_mat = jnp.tril(l_full) * row_scale[:, None]
    b_mat = jax.random.normal(key_b, (N, M), jnp.float32)
    return {'l_mat': l_mat.astype(jnp.bfloat16), 'b_mat': b_mat.astype(jnp.bfloat16)}


def reference(l_mat, b_mat):
    product = jnp.dot(l_mat, b_mat, preferred_element_type=jnp.float32)
    return product.astype(jnp.bfloat16)
```

```python
import functools

import jax
import jax.numpy as jnp
import numpy as np
from jax import lax
from jax.experimental import pallas as pl
from jax.experimental.pallas import tpu as pltpu
from jax.sharding import PartitionSpec as P


TM = 512
KB = 1024
NBUF = 8
WIDTHS = (512, 1024, 1024, 512, 512, 256, 256)


def plan(half):
    tables = []
    for row in range(2):
        steps, seen = [], set()
        for r in range(half // TM):
            n_k = row * (half // KB) + -(-(r + 1) * TM // KB)
            for k in range(n_k):
                steps.append((r, k, int(k == 0), int(k == n_k - 1), int(k not in seen)))
                seen.add(k)
        tables.append(steps)
    return tables


def chunk_kernel(half, depth, col0, width, counts, tab, info, l0, l1, l2, l3, b_loc, b_rec, *rest):
    x_out, bv, lv, acc, ov, lsem, bsem, osem = rest[-8:]
    row, col = info[0], info[1]
    stride = max(counts) * 5
    n = jnp.where(row == 0, counts[0], counts[1])
    per = depth // KB
    nb = half // KB

    def field(t, f):
        return tab[row * stride + t * 5 + f]

    def l_start(t, slot):
        r, k = field(t, 0), field(t, 1)
        which = lax.bitwise_xor(k // per, col)
        for i, ref in enumerate((l0, l1, l2, l3)):
            @pl.when(which == i)
            def _():
                pltpu.make_async_copy(
                    ref.at[pl.ds(r * TM, TM), pl.ds(lax.rem(k, per) * KB, KB)],
                    lv.at[slot], lsem.at[slot]).start()

    def b_copy(ref, src, dst):
        return pltpu.make_async_copy(
            ref.at[pl.ds(src * KB, KB), pl.ds(col0 if ref is b_loc else 0, width)],
            bv.at[pl.ds(dst * KB, KB), :], bsem.at[dst])

    def o_copy(r, slot):
        return pltpu.make_async_copy(
            ov.at[slot], x_out.at[pl.ds(r * TM, TM), pl.ds(col0, width)], osem.at[slot])

    for k in range(nb):
        @pl.when(row == 0)
        def _():
            b_copy(b_loc, k, k).start()

        @pl.when(row == 1)
        def _():
            b_copy(b_rec, k, k).start()

        l_start(k, k)
    for k in range(nb):
        @pl.when(row == 1)
        def _():
            b_copy(b_loc, k, nb + k).start()
    for t in range(nb, NBUF - 1):
        l_start(t, t)

    def step(t, _):
        slot = lax.rem(t, NBUF)
        r, k = field(t, 0), field(t, 1)

        @pl.when(t + NBUF - 1 < n)
        def _():
            l_start(t + NBUF - 1, lax.rem(t + NBUF - 1, NBUF))

        @pl.when(field(t, 4) == 1)
        def _():
            pltpu.make_async_copy(b_loc.at[pl.ds(0, KB), pl.ds(col0, width)],
                                  bv.at[pl.ds(0, KB), :], bsem.at[k]).wait()

        pltpu.make_async_copy(l0.at[pl.ds(0, TM), pl.ds(0, KB)], lv.at[slot], lsem.at[slot]).wait()

        part = functools.partial(jnp.dot, preferred_element_type=jnp.float32)
        first = field(t, 2)
        rows_k = pl.ds(pl.multiple_of(k * KB, KB), KB)

        @pl.when(first == 1)
        def _():
            acc[...] = part(lv[slot], bv[rows_k, :])

        @pl.when(first == 0)
        def _():
            acc[...] += part(lv[slot], bv[rows_k, :])

        @pl.when(field(t, 3) == 1)
        def _():
            oslot = lax.rem(r, 2)

            @pl.when(r >= 2)
            def _():
                o_copy(r - 2, oslot).wait()

            ov[oslot] = acc[...].astype(ov.dtype)
            o_copy(r, oslot).start()

        return 0

    lax.fori_loop(0, n, step, 0)
    last = half // TM
    o_copy(last - 2, (last - 2) % 2).wait()
    o_copy(last - 1, (last - 1) % 2).wait()


def solution(mesh):
    block_spec = P(('batch', 'row'), 'col')
    x_swap = [(0, 2), (1, 3), (2, 0), (3, 1)]
    core_swap = [(0, 1), (1, 0), (2, 3), (3, 2)]

    def product(l_block, b_block):
        half, depth = l_block.shape
        tables = plan(half)
        counts = tuple(len(s) for s in tables)
        flat = np.zeros((2, max(counts), 5), np.int32)
        for row in range(2):
            flat[row, :counts[row]] = tables[row]
        tab = jnp.asarray(flat.reshape(-1))
        info = jnp.stack([lax.axis_index('row'), lax.axis_index('col')]).astype(jnp.int32)

        lc = lax.ppermute(l_block, 'col', core_swap)
        lx = lax.ppermute(l_block, 'col', x_swap)
        recv, col0, source = [], 0, b_block
        for width in WIDTHS:
            piece = source[:, col0:col0 + width]
            piece, source = lax.optimization_barrier((piece, source))
            recv.append(lax.ppermute(piece, 'row', [(0, 1)]))
            col0 += width
        lxc = lax.ppermute(lx, 'col', core_swap)

        x, col0 = None, 0
        for j, width in enumerate(WIDTHS):
            hbm = pl.BlockSpec(memory_space=pltpu.HBM)
            operands = [tab, info, l_block, lc, lx, lxc, b_block, recv[j]]
            if x is not None:
                operands.append(x)
            x = pl.pallas_call(
                functools.partial(chunk_kernel, half, depth, col0, width, counts),
                out_shape=jax.ShapeDtypeStruct(b_block.shape, b_block.dtype),
                grid_spec=pltpu.PrefetchScalarGridSpec(
                    num_scalar_prefetch=2, grid=(1,),
                    in_specs=[hbm] * (len(operands) - 2), out_specs=hbm,
                    scratch_shapes=[
                        pltpu.VMEM((2 * half, width), b_block.dtype),
                        pltpu.VMEM((NBUF, TM, KB), l_block.dtype),
                        pltpu.VMEM((TM, width), jnp.float32),
                        pltpu.VMEM((2, TM, width), b_block.dtype),
                        pltpu.SemaphoreType.DMA((NBUF,)),
                        pltpu.SemaphoreType.DMA((2 * half // KB,)),
                        pltpu.SemaphoreType.DMA((2,)),
                    ]),
                input_output_aliases={} if j == 0 else {8: 0},
                cost_estimate=pl.CostEstimate(flops=max(counts) * 2 * TM * KB * width,
                                              bytes_accessed=max(counts) * 2 * TM * KB, transcendentals=0),
            )(*operands)
            col0 += width
        return x

    return jax.shard_map(product, mesh=mesh, in_specs=(block_spec, block_spec), out_specs=block_spec, check_vma=False)
```

```python
import functools

import jax
import jax.numpy as jnp
import numpy as np
from jax import lax
from jax.experimental import pallas as pl
from jax.experimental.pallas import tpu as pltpu
from jax.sharding import PartitionSpec as P


TM = 1024
KB = 1024
NBUF = 6
FIELDS = 6
WIDTHS = (512, 1024, 1024, 512, 512)
FIRST = (384, 640)
TAIL = (2048, 1024, 512, 512)
SPLIT = 2
KEEP = 1024
DOT = functools.partial(jnp.dot, preferred_element_type=jnp.float32)


def plan(half, with_off):
    tables, nb = [], half // KB
    for row in range(2):
        start = row * nb
        steps, seen = [], set()
        for r in range(half // TM):
            ks = list(range(0 if with_off else start, start + -(-(r + 1) * TM // KB)))
            for k in ks:
                slot = k if with_off else k - start
                steps.append((r, k, int(k == ks[0]), int(k == ks[-1]), int(k not in seen), slot))
                seen.add(k)
        tables.append(steps)
    counts = tuple(len(s) for s in tables)
    flat = np.zeros((2, max(counts), FIELDS), np.int32)
    for row in range(2):
        flat[row, :counts[row]] = tables[row]
    return counts, jnp.asarray(flat.reshape(-1))


def chunk_kernel(half, depth, src0, dst0, width, counts, cuts, n_alias, tab, info, l0, l1, l2, l3, b_loc, *rest):
    pieces = rest[:len(cuts)]
    rest = rest[len(cuts) + n_alias:]
    off = bool(cuts)
    if off:
        out, bv, lv, acc, ov, lsem, bsem, osem = rest
    else:
        out, keep, bv, lv, acc, lsem, bsem, ksem = rest
    row, col = info[0], info[1]
    stride = max(counts) * FIELDS
    n = jnp.where(row == 0, counts[0], counts[1])
    per, nb = depth // KB, half // KB

    def field(t, f):
        return tab[row * stride + t * FIELDS + f]

    def l_start(t, slot):
        r, k = field(t, 0), field(t, 1)
        which = lax.bitwise_xor(k // per, col)
        for i, ref in enumerate((l0, l1, l2, l3)):
            @pl.when(which == i)
            def _():
                pltpu.make_async_copy(
                    ref.at[pl.ds(r * TM, TM), pl.ds(lax.rem(k, per) * KB, KB)],
                    lv.at[slot], lsem.at[slot]).start()

    def b_local(k, slot):
        return pltpu.make_async_copy(
            b_loc.at[pl.ds(k * KB, KB), pl.ds(src0, width)], bv.at[pl.ds(slot * KB, KB), :], bsem.at[slot])

    def b_recv_start(k):
        for ref, cut in zip(pieces, cuts):
            lo, hi = max(k * KB, cut), min((k + 1) * KB, cut + ref.shape[0])
            if lo < hi:
                pltpu.make_async_copy(
                    ref.at[pl.ds(lo - cut, hi - lo), :], bv.at[pl.ds(lo, hi - lo), :], bsem.at[k]).start()

    def o_copy(r, slot):
        return pltpu.make_async_copy(
            ov.at[slot], out.at[pl.ds(r * TM, TM), pl.ds(dst0, width)], osem.at[slot])

    def keep_copy(ref):
        return pltpu.make_async_copy(ref.at[:, pl.ds((half - KEEP) % depth, KEEP)], keep, ksem)

    for k in range(nb):
        if off:
            @pl.when(row == 0)
            def _():
                b_local(k, k).start()

            @pl.when(row == 1)
            def _():
                b_recv_start(k)
        else:
            b_local(k, k).start()
        l_start(k, k)
    if off:
        for k in range(nb):
            @pl.when(row == 1)
            def _():
                b_local(k, nb + k).start()
    for t in range(nb, NBUF - 1):
        l_start(t, t)
    if not off:
        kept = lax.bitwise_xor((half - KEEP) // depth, col)
        for i, ref in enumerate((l0, l1, l2, l3)):
            @pl.when((row == 1) & (kept == i))
            def _():
                keep_copy(ref).start()

    def step(t, _):
        slot = lax.rem(t, NBUF)
        r, at = field(t, 0), field(t, 5)

        @pl.when(t + NBUF - 1 < n)
        def _():
            l_start(t + NBUF - 1, lax.rem(t + NBUF - 1, NBUF))

        @pl.when(field(t, 4) == 1)
        def _():
            b_local(0, at).wait()

        pltpu.make_async_copy(l0.at[pl.ds(0, TM), pl.ds(0, KB)], lv.at[slot], lsem.at[slot]).wait()
        rows_k = pl.ds(pl.multiple_of(at * KB, KB), KB)
        first = field(t, 2)

        @pl.when(first == 1)
        def _():
            acc[...] = DOT(lv[slot], bv[rows_k, :])

        @pl.when(first == 0)
        def _():
            acc[...] += DOT(lv[slot], bv[rows_k, :])

        @pl.when(field(t, 3) == 1)
        def _():
            if off:
                oslot = lax.rem(r, 2)

                @pl.when(r >= 2)
                def _():
                    o_copy(r - 2, oslot).wait()

                ov[oslot] = acc[...].astype(ov.dtype)
                o_copy(r, oslot).start()
            else:
                out[pl.ds(pl.multiple_of(r * TM, TM), TM), :] = acc[...]

        return 0

    lax.fori_loop(0, n, step, 0)
    if off:
        last = half // TM
        o_copy(last - 2, (last - 2) % 2).wait()
        o_copy(last - 1, (last - 1) % 2).wait()
    else:
        @pl.when(row == 1)
        def _():
            keep_copy(l0).wait()


def tail_kernel(half, depth, k0, kw, src0, dst0, width, final, info, part, piece, *rest):
    row, col = info[0], info[1]
    tiles = half // TM
    kept = k0 >= half - KEEP
    if final:
        keep, (out, ov, osem) = rest[0], rest[-3:]
    elif kept:
        keep, out = rest
    else:
        l_refs, (out, bv, lv, lsem, bsem) = rest[:4], rest[4:]
    which = lax.bitwise_xor(k0 // depth, col)

    def l_copy(ref, t):
        slot = lax.rem(t, 2)
        return pltpu.make_async_copy(
            ref.at[pl.ds(t * TM, TM), pl.ds(k0 % depth, kw)], lv.at[slot], lsem.at[slot])

    def l_start(t):
        for i, ref in enumerate(l_refs):
            @pl.when(which == i)
            def _():
                l_copy(ref, t).start()

    def o_copy(t):
        return pltpu.make_async_copy(
            ov.at[t], out.at[pl.ds(t * TM, TM), pl.ds(dst0, width)], osem.at[t])

    def put(t, rows, total):
        if final:
            ov[t] = total.astype(ov.dtype)
            o_copy(t).start()
        else:
            out[rows, :] = total

    @pl.when(row == 1)
    def _():
        if not kept:
            b_copy = pltpu.make_async_copy(piece, bv, bsem)
            b_copy.start()
            l_start(0)
            l_start(1)
            b_copy.wait()
        right = piece if kept else bv

        def add(t, _):
            rows = pl.ds(pl.multiple_of(t * TM, TM), TM)
            if kept:
                tile = keep[rows, pl.ds(k0 - (half - KEEP), kw)]
            else:
                l_copy(l_refs[0], t).wait()
                tile = lv[lax.rem(t, 2)]
            put(t, rows, part[rows, pl.ds(src0, width)] + DOT(tile, right[...]))
            if not kept:
                @pl.when(t + 2 < tiles)
                def _():
                    l_start(t + 2)
            return 0

        lax.fori_loop(0, tiles, add, 0, unroll=kept)

    @pl.when(row == 0)
    def _():
        def move(t, _):
            rows = pl.ds(pl.multiple_of(t * TM, TM), TM)
            put(t, rows, part[rows, pl.ds(src0, width)])
            return 0

        lax.fori_loop(0, tiles, move, 0)

    if final:
        for t in range(tiles):
            o_copy(t).wait()


def solution(mesh):
    block_spec = P(('batch', 'row'), 'col')
    x_swap = [(0, 2), (1, 3), (2, 0), (3, 1)]
    core_swap = [(0, 1), (1, 0), (2, 3), (3, 2)]
    n_first = len(FIRST) + 1
    hbm = pl.BlockSpec(memory_space=pltpu.HBM)
    vmem = pl.BlockSpec(memory_space=pltpu.VMEM)
    smem = pl.BlockSpec(memory_space=pltpu.SMEM)

    def in_hbm(array):
        return pltpu.with_memory_space_constraint(array, pltpu.HBM)

    def product(l_block, b_block):
        half, depth = l_block.shape
        dtype = b_block.dtype
        off_counts, off_tab = plan(half, True)
        diag_counts, diag_tab = plan(half, False)
        info = jnp.stack([lax.axis_index('row'), lax.axis_index('col')]).astype(jnp.int32)
        starts = np.cumsum((0,) + WIDTHS).tolist()
        tail0, tail_w = starts[-1], b_block.shape[1] - starts[-1]

        cuts0 = np.cumsum((0,) + FIRST).tolist()
        boxes = [(r, e - r, 0, WIDTHS[0]) for r, e in zip(cuts0, cuts0[1:] + [half])]
        boxes += [(0, half, c, w) for c, w in zip(starts[1:], WIDTHS[1:])]
        n_main = len(boxes)
        ends = np.cumsum(TAIL).tolist()
        boxes += [(e - h, h, tail0, tail_w) for e, h in zip(ends[:-1], TAIL)]
        last_w = tail_w // SPLIT
        boxes += [(half - TAIL[-1], TAIL[-1], tail0 + i * last_w, last_w) for i in range(SPLIT)]
        recv, source = [], b_block

        def send(j, source):
            r, h, c, w = boxes[j]
            piece = source[r:r + h, c:c + w]
            piece, source = lax.optimization_barrier((piece, source))
            recv.append(lax.ppermute(piece, 'row', [(0, 1), (1, 0)] if j == 0 else [(0, 1)]))
            return source

        n_early = len(boxes) - SPLIT - 1
        for j in range(n_early):
            source = send(j, source)
        lx = lax.ppermute(l_block, 'col', x_swap)
        lc = lax.ppermute(l_block, 'col', core_swap)
        lxc = lax.ppermute(lx, 'col', core_swap)
        l_refs = [l_block, lc, lx, lxc]

        def chunk(pieces, cuts, x, src0, dst0, width, counts, tab):
            alias = [] if x is None else [x]
            operands = [tab, info, *map(in_hbm, [*l_refs, b_block, *pieces]), *alias]
            scratch = [
                pltpu.VMEM(((2 if cuts else 1) * half, width), dtype),
                pltpu.VMEM((NBUF, TM, KB), dtype),
                pltpu.VMEM((TM, width), jnp.float32),
            ]
            sems = [pltpu.SemaphoreType.DMA((NBUF,)), pltpu.SemaphoreType.DMA((2 * half // KB,))]
            if cuts:
                out, out_spec = jax.ShapeDtypeStruct(b_block.shape, dtype), hbm
                scratch += [pltpu.VMEM((2, TM, width), dtype), *sems, pltpu.SemaphoreType.DMA((2,))]
            else:
                out = (pltpu.VMEM((half, width), jnp.float32), pltpu.VMEM((half, KEEP), dtype))
                out_spec = (vmem, vmem)
                scratch += [*sems, pltpu.SemaphoreType.DMA]
            limit = 2 * (NBUF * TM * KB + (2 if cuts else 1) * half * width + 6 * TM * width) + 2 * 2**20
            return pl.pallas_call(
                functools.partial(chunk_kernel, half, depth, src0, dst0, width, counts, cuts, len(alias)),
                out_shape=out,
                in_specs=[smem, smem] + [hbm] * (len(operands) - 2), out_specs=out_spec,
                scratch_shapes=scratch,
                input_output_aliases={len(operands) - 1: 0} if alias else {},
                compiler_params=pltpu.CompilerParams(vmem_limit_bytes=limit),
                cost_estimate=pl.CostEstimate(flops=max(counts) * 2 * TM * KB * width,
                                              bytes_accessed=max(counts) * 2 * TM * KB, transcendentals=0),
            )(*operands)

        def tail(keep, piece, part, x, k0, kw, src0, width):
            final, kept = x is not None, k0 >= half - KEEP
            operands = [info, part, pltpu.with_memory_space_constraint(piece, pltpu.VMEM) if kept else in_hbm(piece)]
            operands += [keep] if kept else list(map(in_hbm, l_refs))
            specs = [smem, vmem] + ([vmem, vmem] if kept else [hbm] * 5)
            scratch, need = [], 4 * TM * width + 2 * 2**20
            if final:
                operands.append(x)
                specs.append(hbm)
                out, out_spec = jax.ShapeDtypeStruct(x.shape, x.dtype), hbm
                scratch = [pltpu.VMEM((half // TM, TM, width), dtype), pltpu.SemaphoreType.DMA((half // TM,))]
                need += 2 * half * width
            else:
                out, out_spec = pltpu.VMEM(part.shape, part.dtype), vmem
                if not kept:
                    scratch = [pltpu.VMEM((kw, width), dtype), pltpu.VMEM((2, TM, kw), dtype),
                               pltpu.SemaphoreType.DMA((2,)), pltpu.SemaphoreType.DMA]
                    need += 2 * kw * (width + 2 * TM)
            return pl.pallas_call(
                functools.partial(tail_kernel, half, depth, k0, kw, src0, tail0 + src0, width, final),
                out_shape=out,
                in_specs=specs, out_specs=out_spec,
                scratch_shapes=scratch,
                input_output_aliases={len(operands) - 1: 0} if final else {1: 0},
                compiler_params=pltpu.CompilerParams(vmem_limit_bytes=need),
                cost_estimate=pl.CostEstimate(flops=2 * half * kw * width,
                                              bytes_accessed=2 * half * kw, transcendentals=0),
            )(*operands)

        x, part = None, None
        for j, width in enumerate(WIDTHS):
            if j == len(WIDTHS) - 1:
                x, b_block = lax.optimization_barrier((x, b_block))
                source = b_block
                for i in range(n_early, len(boxes)):
                    source = send(i, source)
                part, keep = chunk([], (), None, tail0, 0, tail_w, diag_counts, diag_tab)
                x, part, keep = lax.optimization_barrier((x, part, keep))
            pieces, cuts = (recv[:n_first], tuple(cuts0)) if j == 0 else ([recv[n_first - 1 + j]], (0,))
            x = chunk(pieces, cuts, x, starts[j], starts[j], width, off_counts, off_tab)
        x, part = lax.optimization_barrier((x, part))
        for j, (piece, (k0, kw, c, w)) in enumerate(zip(recv[n_main:], boxes[n_main:])):
            final = j >= len(TAIL) - 1
            done = tail(keep, piece, part, x if final else None, k0, kw, c - tail0, w)
            part, x = (part, done) if final else (done, x)
        return x

    return jax.shard_map(product, mesh=mesh, in_specs=(block_spec, block_spec), out_specs=block_spec, check_vma=False)
```

```python
import functools

import jax
import jax.numpy as jnp
import numpy as np
from jax import lax
from jax.experimental import pallas as pl
from jax.experimental.pallas import tpu as pltpu
from jax.sharding import PartitionSpec as P


TM = 1024
KB = 1024
NBUF = 6
FIELDS = 6
WIDTHS = (512, 1024, 1024, 512, 512)
FIRST = (384, 640)
TAIL = (2048, 1024, 512, 512)
SPLIT = 2
KEEP = 1024
DOT = functools.partial(jnp.dot, preferred_element_type=jnp.float32)


def plan(half, with_off):
    tables, nb = [], half // KB
    for row in range(2):
        start = row * nb
        steps, seen = [], set()
        for r in range(half // TM):
            ks = list(range(0 if with_off else start, start + -(-(r + 1) * TM // KB)))
            for k in ks:
                slot = k if with_off else k - start
                steps.append((r, k, int(k == ks[0]), int(k == ks[-1]), int(k not in seen), slot))
                seen.add(k)
        tables.append(steps)
    counts = tuple(len(s) for s in tables)
    flat = np.zeros((2, max(counts), FIELDS), np.int32)
    for row in range(2):
        flat[row, :counts[row]] = tables[row]
    return counts, jnp.asarray(flat.reshape(-1))


def chunk_kernel(half, depth, src0, dst0, width, counts, cuts, n_alias, tab, info, l0, l1, l2, l3, b_loc, *rest):
    pieces = rest[:len(cuts)]
    rest = rest[len(cuts) + n_alias:]
    off = bool(cuts)
    if off:
        out, bv, lv, acc, ov, lsem, bsem, osem = rest
    else:
        out, keep, bv, lv, acc, lsem, bsem, ksem = rest
    row, col = info[0], info[1]
    stride = max(counts) * FIELDS
    n = jnp.where(row == 0, counts[0], counts[1])
    per, nb = depth // KB, half // KB

    def field(t, f):
        return tab[row * stride + t * FIELDS + f]

    def l_start(t, slot):
        r, k = field(t, 0), field(t, 1)
        which = lax.bitwise_xor(k // per, col)
        for i, ref in enumerate((l0, l1, l2, l3)):
            @pl.when(which == i)
            def _():
                pltpu.make_async_copy(
                    ref.at[pl.ds(r * TM, TM), pl.ds(lax.rem(k, per) * KB, KB)],
                    lv.at[slot], lsem.at[slot]).start()

    def b_local(k, slot):
        return pltpu.make_async_copy(
            b_loc.at[pl.ds(k * KB, KB), pl.ds(src0, width)], bv.at[pl.ds(slot * KB, KB), :], bsem.at[slot])

    def b_recv_start(k):
        for ref, cut in zip(pieces, cuts):
            lo, hi = max(k * KB, cut), min((k + 1) * KB, cut + ref.shape[0])
            if lo < hi:
                pltpu.make_async_copy(
                    ref.at[pl.ds(lo - cut, hi - lo), :], bv.at[pl.ds(lo, hi - lo), :], bsem.at[k]).start()

    def o_copy(r, slot):
        return pltpu.make_async_copy(
            ov.at[slot], out.at[pl.ds(r * TM, TM), pl.ds(dst0, width)], osem.at[slot])

    def keep_copy(ref):
        return pltpu.make_async_copy(ref.at[:, pl.ds((half - KEEP) % depth, KEEP)], keep, ksem)

    for k in range(nb):
        if off:
            @pl.when(row == 0)
            def _():
                b_local(k, k).start()

            @pl.when(row == 1)
            def _():
                b_recv_start(k)
        else:
            b_local(k, k).start()
        l_start(k, k)
    if off:
        for k in range(nb):
            @pl.when(row == 1)
            def _():
                b_local(k, nb + k).start()
    for t in range(nb, NBUF - 1):
        l_start(t, t)
    if not off:
        kept = lax.bitwise_xor((half - KEEP) // depth, col)
        for i, ref in enumerate((l0, l1, l2, l3)):
            @pl.when((row == 1) & (kept == i))
            def _():
                keep_copy(ref).start()

    def step(t, _):
        slot = lax.rem(t, NBUF)
        r, at = field(t, 0), field(t, 5)

        @pl.when(t + NBUF - 1 < n)
        def _():
            l_start(t + NBUF - 1, lax.rem(t + NBUF - 1, NBUF))

        @pl.when(field(t, 4) == 1)
        def _():
            b_local(0, at).wait()

        pltpu.make_async_copy(l0.at[pl.ds(0, TM), pl.ds(0, KB)], lv.at[slot], lsem.at[slot]).wait()
        rows_k = pl.ds(pl.multiple_of(at * KB, KB), KB)
        first = field(t, 2)

        @pl.when(first == 1)
        def _():
            acc[...] = DOT(lv[slot], bv[rows_k, :])

        @pl.when(first == 0)
        def _():
            acc[...] += DOT(lv[slot], bv[rows_k, :])

        @pl.when(field(t, 3) == 1)
        def _():
            if off:
                oslot = lax.rem(r, 2)

                @pl.when(r >= 2)
                def _():
                    o_copy(r - 2, oslot).wait()

                ov[oslot] = acc[...].astype(ov.dtype)
                o_copy(r, oslot).start()
            else:
                out[pl.ds(pl.multiple_of(r * TM, TM), TM), :] = acc[...]

        return 0

    lax.fori_loop(0, n, step, 0)
    if off:
        last = half // TM
        o_copy(last - 2, (last - 2) % 2).wait()
        o_copy(last - 1, (last - 1) % 2).wait()
    else:
        @pl.when(row == 1)
        def _():
            keep_copy(l0).wait()


def tail_kernel(half, depth, k0, kw, src0, dst0, width, final, part, piece, *rest):
    row, col = lax.axis_index('row'), lax.axis_index('col')
    tiles = half // TM
    kept = k0 >= half - KEEP
    if final:
        keep, (out, ov, osem) = rest[0], rest[-3:]
    elif kept:
        keep, out = rest
    else:
        l_refs, (out, bv, lv, lsem, bsem) = rest[:4], rest[4:]
    which = lax.bitwise_xor(k0 // depth, col)

    def l_copy(ref, t):
        slot = lax.rem(t, 2)
        return pltpu.make_async_copy(
            ref.at[pl.ds(t * TM, TM), pl.ds(k0 % depth, kw)], lv.at[slot], lsem.at[slot])

    def l_start(t):
        for i, ref in enumerate(l_refs):
            @pl.when(which == i)
            def _():
                l_copy(ref, t).start()

    def o_copy(t):
        return pltpu.make_async_copy(
            ov.at[t], out.at[pl.ds(t * TM, TM), pl.ds(dst0, width)], osem.at[t])

    def put(t, rows, total):
        if final:
            ov[t] = total.astype(ov.dtype)
            o_copy(t).start()
        else:
            out[rows, :] = total

    @pl.when(row == 1)
    def _():
        if not kept:
            b_copy = pltpu.make_async_copy(piece, bv, bsem)
            b_copy.start()
            l_start(0)
            l_start(1)
            b_copy.wait()
        right = piece if kept else bv

        def add(t, _):
            rows = pl.ds(pl.multiple_of(t * TM, TM), TM)
            if kept:
                tile = keep[rows, pl.ds(k0 - (half - KEEP), kw)]
            else:
                l_copy(l_refs[0], t).wait()
                tile = lv[lax.rem(t, 2)]
            put(t, rows, part[rows, pl.ds(src0, width)] + DOT(tile, right[...]))
            if not kept:
                @pl.when(t + 2 < tiles)
                def _():
                    l_start(t + 2)
            return 0

        lax.fori_loop(0, tiles, add, 0, unroll=kept)

    @pl.when(row == 0)
    def _():
        def move(t, _):
            rows = pl.ds(pl.multiple_of(t * TM, TM), TM)
            put(t, rows, part[rows, pl.ds(src0, width)])
            return 0

        lax.fori_loop(0, tiles, move, 0)

    if final:
        for t in range(tiles):
            o_copy(t).wait()


def solution(mesh):
    block_spec = P(('batch', 'row'), 'col')
    x_swap = [(0, 2), (1, 3), (2, 0), (3, 1)]
    core_swap = [(0, 1), (1, 0), (2, 3), (3, 2)]
    n_first = len(FIRST) + 1
    hbm = pl.BlockSpec(memory_space=pltpu.HBM)
    vmem = pl.BlockSpec(memory_space=pltpu.VMEM)
    smem = pl.BlockSpec(memory_space=pltpu.SMEM)

    def in_hbm(array):
        return pltpu.with_memory_space_constraint(array, pltpu.HBM)

    def product(l_block, b_block):
        half, depth = l_block.shape
        dtype = b_block.dtype
        off_counts, off_tab = plan(half, True)
        diag_counts, diag_tab = plan(half, False)
        info = jnp.stack([lax.axis_index('row'), lax.axis_index('col')]).astype(jnp.int32)
        starts = np.cumsum((0,) + WIDTHS).tolist()
        tail0, tail_w = starts[-1], b_block.shape[1] - starts[-1]

        cuts0 = np.cumsum((0,) + FIRST).tolist()
        boxes = [(r, e - r, 0, WIDTHS[0]) for r, e in zip(cuts0, cuts0[1:] + [half])]
        boxes += [(0, half, c, w) for c, w in zip(starts[1:], WIDTHS[1:])]
        n_main = len(boxes)
        ends = np.cumsum(TAIL).tolist()
        boxes += [(e - h, h, tail0, tail_w) for e, h in zip(ends[:-1], TAIL)]
        last_w = tail_w // SPLIT
        boxes += [(half - TAIL[-1], TAIL[-1], tail0 + i * last_w, last_w) for i in range(SPLIT)]
        recv, source = [], b_block

        def send(j, source):
            r, h, c, w = boxes[j]
            piece = source[r:r + h, c:c + w]
            piece, source = lax.optimization_barrier((piece, source))
            recv.append(lax.ppermute(piece, 'row', [(0, 1), (1, 0)] if j == 0 else [(0, 1)]))
            return source

        n_early = len(boxes) - SPLIT - 1
        for j in range(n_early):
            source = send(j, source)
        lx = lax.ppermute(l_block, 'col', x_swap)
        lc = lax.ppermute(l_block, 'col', core_swap)
        lxc = lax.ppermute(lx, 'col', core_swap)
        l_refs = [l_block, lc, lx, lxc]

        def chunk(pieces, cuts, x, src0, dst0, width, counts, tab):
            alias = [] if x is None else [x]
            operands = [tab, info, *map(in_hbm, [*l_refs, b_block, *pieces]), *alias]
            scratch = [
                pltpu.VMEM(((2 if cuts else 1) * half, width), dtype),
                pltpu.VMEM((NBUF, TM, KB), dtype),
                pltpu.VMEM((TM, width), jnp.float32),
            ]
            sems = [pltpu.SemaphoreType.DMA((NBUF,)), pltpu.SemaphoreType.DMA((2 * half // KB,))]
            if cuts:
                out, out_spec = jax.ShapeDtypeStruct(b_block.shape, dtype), hbm
                scratch += [pltpu.VMEM((2, TM, width), dtype), *sems, pltpu.SemaphoreType.DMA((2,))]
            else:
                out = (pltpu.VMEM((half, width), jnp.float32), pltpu.VMEM((half, KEEP), dtype))
                out_spec = (vmem, vmem)
                scratch += [*sems, pltpu.SemaphoreType.DMA]
            limit = 2 * (NBUF * TM * KB + (2 if cuts else 1) * half * width + 6 * TM * width) + 2 * 2**20
            return pl.pallas_call(
                functools.partial(chunk_kernel, half, depth, src0, dst0, width, counts, cuts, len(alias)),
                out_shape=out,
                in_specs=[smem, smem] + [hbm] * (len(operands) - 2), out_specs=out_spec,
                scratch_shapes=scratch,
                input_output_aliases={len(operands) - 1: 0} if alias else {},
                compiler_params=pltpu.CompilerParams(vmem_limit_bytes=limit),
                cost_estimate=pl.CostEstimate(flops=max(counts) * 2 * TM * KB * width,
                                              bytes_accessed=max(counts) * 2 * TM * KB, transcendentals=0),
            )(*operands)

        def tail(keep, piece, part, x, k0, kw, src0, width):
            final, kept = x is not None, k0 >= half - KEEP
            operands = [part, pltpu.with_memory_space_constraint(piece, pltpu.VMEM) if kept else in_hbm(piece)]
            operands += [keep] if kept else list(map(in_hbm, l_refs))
            specs = [vmem] + ([vmem, vmem] if kept else [hbm] * 5)
            scratch, need = [], 4 * TM * width + 2 * 2**20
            if final:
                operands.append(x)
                specs.append(hbm)
                out, out_spec = jax.ShapeDtypeStruct(x.shape, x.dtype), hbm
                scratch = [pltpu.VMEM((half // TM, TM, width), dtype), pltpu.SemaphoreType.DMA((half // TM,))]
                need += 2 * half * width
            else:
                out, out_spec = pltpu.VMEM(part.shape, part.dtype), vmem
                if not kept:
                    scratch = [pltpu.VMEM((kw, width), dtype), pltpu.VMEM((2, TM, kw), dtype),
                               pltpu.SemaphoreType.DMA((2,)), pltpu.SemaphoreType.DMA]
                    need += 2 * kw * (width + 2 * TM)
            return pl.pallas_call(
                functools.partial(tail_kernel, half, depth, k0, kw, src0, tail0 + src0, width, final),
                out_shape=out,
                in_specs=specs, out_specs=out_spec,
                scratch_shapes=scratch,
                input_output_aliases={len(operands) - 1: 0} if final else {0: 0},
                compiler_params=pltpu.CompilerParams(vmem_limit_bytes=need),
                cost_estimate=pl.CostEstimate(flops=2 * half * kw * width,
                                              bytes_accessed=2 * half * kw, transcendentals=0),
            )(*operands)

        x, part = None, None
        for j, width in enumerate(WIDTHS):
            if j == len(WIDTHS) - 1:
                x, b_block = lax.optimization_barrier((x, b_block))
                source = b_block
                for i in range(n_early, len(boxes)):
                    source = send(i, source)
                part, keep = chunk([], (), None, tail0, 0, tail_w, diag_counts, diag_tab)
                x, part, keep = lax.optimization_barrier((x, part, keep))
            pieces, cuts = (recv[:n_first], tuple(cuts0)) if j == 0 else ([recv[n_first - 1 + j]], (0,))
            x = chunk(pieces, cuts, x, starts[j], starts[j], width, off_counts, off_tab)
        x, part = lax.optimization_barrier((x, part))
        for j, (piece, (k0, kw, c, w)) in enumerate(zip(recv[n_main:], boxes[n_main:])):
            final = j >= len(TAIL) - 1
            done = tail(keep, piece, part, x if final else None, k0, kw, c - tail0, w)
            part, x = (part, done) if final else (done, x)
        return x

    return jax.shard_map(product, mesh=mesh, in_specs=(block_spec, block_spec), out_specs=block_spec, check_vma=False)
```

```python
import functools

import jax
import jax.numpy as jnp
import numpy as np
from jax import lax
from jax.experimental import pallas as pl
from jax.experimental.pallas import tpu as pltpu
from jax.sharding import PartitionSpec as P


TM = 1024
KB = 1024
NBUF = 6
FIELDS = 6
WIDTHS = (512, 1024, 1024, 512, 512)
FIRST = (384, 640)
TAIL = (2048, 1024, 512, 512)
LAST = ((512,), (256, 256))
KEEP = 1024
DOT = functools.partial(jnp.dot, preferred_element_type=jnp.float32)


def plan(half, with_off):
    tables, nb = [], half // KB
    for row in range(2):
        start = row * nb
        steps, seen = [], set()
        for r in range(half // TM):
            ks = list(range(0 if with_off else start, start + -(-(r + 1) * TM // KB)))
            for k in ks:
                slot = k if with_off else k - start
                steps.append((r, k, int(k == ks[0]), int(k == ks[-1]), int(k not in seen), slot))
                seen.add(k)
        tables.append(steps)
    counts = tuple(len(s) for s in tables)
    flat = np.zeros((2, max(counts), FIELDS), np.int32)
    for row in range(2):
        flat[row, :counts[row]] = tables[row]
    return counts, jnp.asarray(flat.reshape(-1))


def chunk_kernel(half, depth, src0, dst0, width, counts, cuts, n_alias, tab, info, l0, l1, l2, l3, b_loc, *rest):
    pieces = rest[:len(cuts)]
    rest = rest[len(cuts) + n_alias:]
    off = bool(cuts)
    if off:
        out, bv, lv, acc, ov, lsem, bsem, osem = rest
    else:
        out, keep, bv, lv, acc, lsem, bsem, ksem = rest
    row, col = info[0], info[1]
    stride = max(counts) * FIELDS
    n = jnp.where(row == 0, counts[0], counts[1])
    per, nb = depth // KB, half // KB

    def field(t, f):
        return tab[row * stride + t * FIELDS + f]

    def l_start(t, slot):
        r, k = field(t, 0), field(t, 1)
        which = lax.bitwise_xor(k // per, col)
        for i, ref in enumerate((l0, l1, l2, l3)):
            @pl.when(which == i)
            def _():
                pltpu.make_async_copy(
                    ref.at[pl.ds(r * TM, TM), pl.ds(lax.rem(k, per) * KB, KB)],
                    lv.at[slot], lsem.at[slot]).start()

    def b_local(k, slot):
        return pltpu.make_async_copy(
            b_loc.at[pl.ds(k * KB, KB), pl.ds(src0, width)], bv.at[pl.ds(slot * KB, KB), :], bsem.at[slot])

    def b_recv_start(k):
        twins = len(cuts) > 1
        ends = (cuts[2:3] + cuts[2:] if twins else ()) + (half,)
        for i, (ref, cut, end) in enumerate(zip(pieces, cuts, ends)):
            lo, hi = max(k * KB, cut), min((k + 1) * KB, end)
            if lo < hi:
                @pl.when(lax.rem(col, 2) == i if twins and i < 2 else True)
                def _():
                    pltpu.make_async_copy(
                        ref.at[pl.ds(lo - cut, hi - lo), :], bv.at[pl.ds(lo, hi - lo), :], bsem.at[k]).start()

    def o_copy(r, slot):
        return pltpu.make_async_copy(
            ov.at[slot], out.at[pl.ds(r * TM, TM), pl.ds(dst0, width)], osem.at[slot])

    def keep_copy(ref):
        return pltpu.make_async_copy(ref.at[:, pl.ds((half - KEEP) % depth, KEEP)], keep, ksem)

    for k in range(nb):
        if off:
            @pl.when(row == 0)
            def _():
                b_local(k, k).start()

            @pl.when(row == 1)
            def _():
                b_recv_start(k)
        else:
            b_local(k, k).start()
        l_start(k, k)
    if off:
        for k in range(nb):
            @pl.when(row == 1)
            def _():
                b_local(k, nb + k).start()
    for t in range(nb, NBUF - 1):
        l_start(t, t)
    if not off:
        kept = lax.bitwise_xor((half - KEEP) // depth, col)
        for i, ref in enumerate((l0, l1, l2, l3)):
            @pl.when((row == 1) & (kept == i))
            def _():
                keep_copy(ref).start()

    def step(t, _):
        slot = lax.rem(t, NBUF)
        r, at = field(t, 0), field(t, 5)

        @pl.when(t + NBUF - 1 < n)
        def _():
            l_start(t + NBUF - 1, lax.rem(t + NBUF - 1, NBUF))

        @pl.when(field(t, 4) == 1)
        def _():
            b_local(0, at).wait()

        pltpu.make_async_copy(l0.at[pl.ds(0, TM), pl.ds(0, KB)], lv.at[slot], lsem.at[slot]).wait()
        rows_k = pl.ds(pl.multiple_of(at * KB, KB), KB)
        first = field(t, 2)

        @pl.when(first == 1)
        def _():
            acc[...] = DOT(lv[slot], bv[rows_k, :])

        @pl.when(first == 0)
        def _():
            acc[...] += DOT(lv[slot], bv[rows_k, :])

        @pl.when(field(t, 3) == 1)
        def _():
            if off:
                oslot = lax.rem(r, 2)

                @pl.when(r >= 2)
                def _():
                    o_copy(r - 2, oslot).wait()

                ov[oslot] = acc[...].astype(ov.dtype)
                o_copy(r, oslot).start()
            else:
                out[pl.ds(pl.multiple_of(r * TM, TM), TM), :] = acc[...]

        return 0

    lax.fori_loop(0, n, step, 0)
    if off:
        last = half // TM
        o_copy(last - 2, (last - 2) % 2).wait()
        o_copy(last - 1, (last - 1) % 2).wait()
    else:
        @pl.when(row == 1)
        def _():
            keep_copy(l0).wait()


def tail_kernel(half, depth, k0, kw, src0, dst0, width, final, part, piece, *rest):
    row, col = lax.axis_index('row'), lax.axis_index('col')
    tiles = half // TM
    kept = k0 >= half - KEEP
    if final:
        keep, (out, ov, osem) = rest[0], rest[-3:]
    elif kept:
        keep, out = rest
    else:
        l_refs, (out, bv, lv, lsem, bsem) = rest[:4], rest[4:]
    which = lax.bitwise_xor(k0 // depth, col)

    def l_copy(ref, t):
        slot = lax.rem(t, 2)
        return pltpu.make_async_copy(
            ref.at[pl.ds(t * TM, TM), pl.ds(k0 % depth, kw)], lv.at[slot], lsem.at[slot])

    def l_start(t):
        for i, ref in enumerate(l_refs):
            @pl.when(which == i)
            def _():
                l_copy(ref, t).start()

    def o_copy(t):
        return pltpu.make_async_copy(
            ov.at[t], out.at[pl.ds(t * TM, TM), pl.ds(dst0, width)], osem.at[t])

    def put(t, rows, total):
        if final:
            ov[t] = total.astype(ov.dtype)
            o_copy(t).start()
        else:
            out[rows, pl.ds(src0, width)] = total

    @pl.when(row == 1)
    def _():
        if not kept:
            b_copy = pltpu.make_async_copy(piece, bv, bsem)
            b_copy.start()
            l_start(0)
            l_start(1)
            b_copy.wait()
        right = piece if kept else bv

        def add(t, _):
            rows = pl.ds(pl.multiple_of(t * TM, TM), TM)
            if kept:
                tile = keep[rows, pl.ds(k0 - (half - KEEP), kw)]
            else:
                l_copy(l_refs[0], t).wait()
                tile = lv[lax.rem(t, 2)]
            put(t, rows, part[rows, pl.ds(src0, width)] + DOT(tile, right[...]))
            if not kept:
                @pl.when(t + 2 < tiles)
                def _():
                    l_start(t + 2)
            return 0

        lax.fori_loop(0, tiles, add, 0, unroll=kept)

    @pl.when(row == 0)
    def _():
        def move(t, _):
            rows = pl.ds(pl.multiple_of(t * TM, TM), TM)
            put(t, rows, part[rows, pl.ds(src0, width)])
            return 0

        lax.fori_loop(0, tiles, move, 0)

    if final:
        for t in range(tiles):
            o_copy(t).wait()


def solution(mesh):
    block_spec = P(('batch', 'row'), 'col')
    x_swap = [(0, 2), (1, 3), (2, 0), (3, 1)]
    core_swap = [(0, 1), (1, 0), (2, 3), (3, 2)]
    n_first = len(FIRST) + 1
    hbm = pl.BlockSpec(memory_space=pltpu.HBM)
    vmem = pl.BlockSpec(memory_space=pltpu.VMEM)
    smem = pl.BlockSpec(memory_space=pltpu.SMEM)

    def in_hbm(array):
        return pltpu.with_memory_space_constraint(array, pltpu.HBM)

    def product(l_block, b_block):
        half, depth = l_block.shape
        dtype = b_block.dtype
        off_counts, off_tab = plan(half, True)
        diag_counts, diag_tab = plan(half, False)
        info = jnp.stack([lax.axis_index('row'), lax.axis_index('col')]).astype(jnp.int32)
        starts = np.cumsum((0,) + WIDTHS).tolist()
        tail0, tail_w = starts[-1], b_block.shape[1] - starts[-1]

        cuts0 = np.cumsum((0,) + FIRST).tolist()
        boxes = [(r, e - r, 0, WIDTHS[0]) for r, e in zip(cuts0, cuts0[1:] + [half])]
        boxes += [(0, half, c, w) for c, w in zip(starts[1:], WIDTHS[1:])]
        n_main = len(boxes)
        ends = np.cumsum(TAIL).tolist()
        boxes += [(e - h, h, tail0, tail_w) for e, h in zip(ends[:-1], TAIL)]
        last_w = tail_w // len(LAST)
        n_early = len(boxes) - 1
        for i, ks in enumerate(LAST):
            boxes += [(half - TAIL[-1] + e - h, h, tail0 + i * last_w, last_w) for e, h in zip(np.cumsum(ks).tolist(), ks)]
        recv, source = [], b_block

        def send(j, source):
            r, h, c, w = boxes[j]
            piece = source[r:r + h, c:c + w]
            piece, source = lax.optimization_barrier((piece, source))
            recv.append(lax.ppermute(piece, 'row', [(0, 1)]))
            return source

        first = []
        for core in range(2):
            piece = source[:FIRST[0], :WIDTHS[0]]
            piece, source = lax.optimization_barrier((piece, source))
            pairs = [(i, (i + 4) % 8 if i % 2 == core else i) for i in range(8)]
            first.append(lax.ppermute(piece, ('row', 'col'), pairs))
        recv.append(None)

        for j in range(1, n_early):
            source = send(j, source)
        lx = lax.ppermute(l_block, 'col', x_swap)
        lc = lax.ppermute(l_block, 'col', core_swap)
        lxc = lax.ppermute(lx, 'col', core_swap)
        l_refs = [l_block, lc, lx, lxc]

        def chunk(pieces, cuts, x, src0, dst0, width, counts, tab):
            alias = [] if x is None else [x]
            operands = [tab, info, *map(in_hbm, [*l_refs, b_block, *pieces]), *alias]
            scratch = [
                pltpu.VMEM(((2 if cuts else 1) * half, width), dtype),
                pltpu.VMEM((NBUF, TM, KB), dtype),
                pltpu.VMEM((TM, width), jnp.float32),
            ]
            sems = [pltpu.SemaphoreType.DMA((NBUF,)), pltpu.SemaphoreType.DMA((2 * half // KB,))]
            if cuts:
                out, out_spec = jax.ShapeDtypeStruct(b_block.shape, dtype), hbm
                scratch += [pltpu.VMEM((2, TM, width), dtype), *sems, pltpu.SemaphoreType.DMA((2,))]
            else:
                out = (pltpu.VMEM((half, width), jnp.float32), pltpu.VMEM((half, KEEP), dtype))
                out_spec = (vmem, vmem)
                scratch += [*sems, pltpu.SemaphoreType.DMA]
            limit = 2 * (NBUF * TM * KB + (2 if cuts else 1) * half * width + 6 * TM * width) + 2 * 2**20
            return pl.pallas_call(
                functools.partial(chunk_kernel, half, depth, src0, dst0, width, counts, cuts, len(alias)),
                out_shape=out,
                in_specs=[smem, smem] + [hbm] * (len(operands) - 2), out_specs=out_spec,
                scratch_shapes=scratch,
                input_output_aliases={len(operands) - 1: 0} if alias else {},
                compiler_params=pltpu.CompilerParams(vmem_limit_bytes=limit),
                cost_estimate=pl.CostEstimate(flops=max(counts) * 2 * TM * KB * width,
                                              bytes_accessed=max(counts) * 2 * TM * KB, transcendentals=0),
            )(*operands)

        def tail(keep, piece, part, x, k0, kw, src0, width):
            final, kept = x is not None, k0 >= half - KEEP
            operands = [part, pltpu.with_memory_space_constraint(piece, pltpu.VMEM) if kept else in_hbm(piece)]
            operands += [keep] if kept else list(map(in_hbm, l_refs))
            specs = [vmem] + ([vmem, vmem] if kept else [hbm] * 5)
            scratch, need = [], 4 * TM * width + 2 * 2**20
            if final:
                operands.append(x)
                specs.append(hbm)
                out, out_spec = jax.ShapeDtypeStruct(x.shape, x.dtype), hbm
                scratch = [pltpu.VMEM((half // TM, TM, width), dtype), pltpu.SemaphoreType.DMA((half // TM,))]
                need += 2 * half * width
            else:
                out, out_spec = pltpu.VMEM(part.shape, part.dtype), vmem
                if not kept:
                    scratch = [pltpu.VMEM((kw, width), dtype), pltpu.VMEM((2, TM, kw), dtype),
                               pltpu.SemaphoreType.DMA((2,)), pltpu.SemaphoreType.DMA]
                    need += 2 * kw * (width + 2 * TM)
            return pl.pallas_call(
                functools.partial(tail_kernel, half, depth, k0, kw, src0, tail0 + src0, width, final),
                out_shape=out,
                in_specs=specs, out_specs=out_spec,
                scratch_shapes=scratch,
                input_output_aliases={len(operands) - 1: 0} if final else {0: 0},
                compiler_params=pltpu.CompilerParams(vmem_limit_bytes=need),
                cost_estimate=pl.CostEstimate(flops=2 * half * kw * width,
                                              bytes_accessed=2 * half * kw, transcendentals=0),
            )(*operands)

        x, part = None, None
        for j, width in enumerate(WIDTHS):
            if j == len(WIDTHS) - 1:
                x, b_block = lax.optimization_barrier((x, b_block))
                source = b_block
                for i in range(n_early, len(boxes)):
                    source = send(i, source)
                part, keep = chunk([], (), None, tail0, 0, tail_w, diag_counts, diag_tab)
                x, part, keep = lax.optimization_barrier((x, part, keep))
            pieces, cuts = (first + recv[1:n_first], (0, 0) + tuple(cuts0[1:])) if j == 0 else ([recv[n_first - 1 + j]], (0,))
            x = chunk(pieces, cuts, x, starts[j], starts[j], width, off_counts, off_tab)
        x, part = lax.optimization_barrier((x, part))
        for piece, (k0, kw, c, w) in zip(recv[n_main:], boxes[n_main:]):
            final = k0 + kw == half
            done = tail(keep, piece, part, x if final else None, k0, kw, c - tail0, w)
            part, x = (part, done) if final else (done, x)
            x, part = lax.optimization_barrier((x, part))
        return x

    return jax.shard_map(product, mesh=mesh, in_specs=(block_spec, block_spec), out_specs=block_spec, check_vma=False)
```

```python
import functools

import jax
import jax.numpy as jnp
import numpy as np
from jax import lax
from jax.experimental import pallas as pl
from jax.experimental.pallas import tpu as pltpu
from jax.sharding import PartitionSpec as P


TM = 1024
KB = 1024
NBUF = 6
FIELDS = 6
WIDTHS = (512, 1024, 1024, 512, 512)
FIRST = (384, 640)
TAIL = (2048, 1024, 512, 512)
LAST = ((256, (512,)), (256, (256, 256)))
KEEP = 1024
DOT = functools.partial(jnp.dot, preferred_element_type=jnp.float32)


def plan(half, with_off):
    tables, nb = [], half // KB
    for row in range(2):
        start = row * nb
        steps, seen = [], set()
        for r in range(half // TM):
            ks = list(range(0 if with_off else start, start + -(-(r + 1) * TM // KB)))
            for k in ks:
                slot = k if with_off else k - start
                steps.append((r, k, int(k == ks[0]), int(k == ks[-1]), int(k not in seen), slot))
                seen.add(k)
        tables.append(steps)
    counts = tuple(len(s) for s in tables)
    flat = np.zeros((2, max(counts), FIELDS), np.int32)
    for row in range(2):
        flat[row, :counts[row]] = tables[row]
    return counts, jnp.asarray(flat.reshape(-1))


def chunk_kernel(half, depth, src0, dst0, width, counts, cuts, n_alias, tab, info, l0, l1, l2, l3, b_loc, *rest):
    pieces = rest[:len(cuts)]
    rest = rest[len(cuts) + n_alias:]
    off = bool(cuts)
    if off:
        out, bv, lv, acc, ov, lsem, bsem, osem = rest
    else:
        out, keep, bv, lv, acc, lsem, bsem, ksem = rest
    row, col = info[0], info[1]
    stride = max(counts) * FIELDS
    n = jnp.where(row == 0, counts[0], counts[1])
    per, nb = depth // KB, half // KB

    def field(t, f):
        return tab[row * stride + t * FIELDS + f]

    def l_start(t, slot):
        r, k = field(t, 0), field(t, 1)
        which = lax.bitwise_xor(k // per, col)
        for i, ref in enumerate((l0, l1, l2, l3)):
            @pl.when(which == i)
            def _():
                pltpu.make_async_copy(
                    ref.at[pl.ds(r * TM, TM), pl.ds(lax.rem(k, per) * KB, KB)],
                    lv.at[slot], lsem.at[slot]).start()

    def b_local(k, slot):
        return pltpu.make_async_copy(
            b_loc.at[pl.ds(k * KB, KB), pl.ds(src0, width)], bv.at[pl.ds(slot * KB, KB), :], bsem.at[slot])

    def b_recv_start(k):
        for ref, cut in zip(pieces, cuts):
            lo, hi = max(k * KB, cut), min((k + 1) * KB, cut + ref.shape[0])
            if lo < hi:
                pltpu.make_async_copy(
                    ref.at[pl.ds(lo - cut, hi - lo), :], bv.at[pl.ds(lo, hi - lo), :], bsem.at[k]).start()

    def o_copy(r, slot):
        return pltpu.make_async_copy(
            ov.at[slot], out.at[pl.ds(r * TM, TM), pl.ds(dst0, width)], osem.at[slot])

    def keep_copy(ref):
        return pltpu.make_async_copy(ref.at[:, pl.ds((half - KEEP) % depth, KEEP)], keep, ksem)

    for k in range(nb):
        if off:
            @pl.when(row == 0)
            def _():
                b_local(k, k).start()

            @pl.when(row == 1)
            def _():
                b_recv_start(k)
        else:
            b_local(k, k).start()
        l_start(k, k)
    if off:
        for k in range(nb):
            @pl.when(row == 1)
            def _():
                b_local(k, nb + k).start()
    for t in range(nb, NBUF - 1):
        l_start(t, t)
    if not off:
        kept = lax.bitwise_xor((half - KEEP) // depth, col)
        for i, ref in enumerate((l0, l1, l2, l3)):
            @pl.when((row == 1) & (kept == i))
            def _():
                keep_copy(ref).start()

    def step(t, _):
        slot = lax.rem(t, NBUF)
        r, at = field(t, 0), field(t, 5)

        @pl.when(t + NBUF - 1 < n)
        def _():
            l_start(t + NBUF - 1, lax.rem(t + NBUF - 1, NBUF))

        @pl.when(field(t, 4) == 1)
        def _():
            b_local(0, at).wait()

        pltpu.make_async_copy(l0.at[pl.ds(0, TM), pl.ds(0, KB)], lv.at[slot], lsem.at[slot]).wait()
        rows_k = pl.ds(pl.multiple_of(at * KB, KB), KB)
        first = field(t, 2)

        @pl.when(first == 1)
        def _():
            acc[...] = DOT(lv[slot], bv[rows_k, :])

        @pl.when(first == 0)
        def _():
            acc[...] += DOT(lv[slot], bv[rows_k, :])

        @pl.when(field(t, 3) == 1)
        def _():
            if off:
                oslot = lax.rem(r, 2)

                @pl.when(r >= 2)
                def _():
                    o_copy(r - 2, oslot).wait()

                ov[oslot] = acc[...].astype(ov.dtype)
                o_copy(r, oslot).start()
            else:
                out[pl.ds(pl.multiple_of(r * TM, TM), TM), :] = acc[...]

        return 0

    lax.fori_loop(0, n, step, 0)
    if off:
        last = half // TM
        o_copy(last - 2, (last - 2) % 2).wait()
        o_copy(last - 1, (last - 1) % 2).wait()
    else:
        @pl.when(row == 1)
        def _():
            keep_copy(l0).wait()


def tail_kernel(half, depth, k0, kw, src0, dst0, width, final, part, piece, *rest):
    row, col = lax.axis_index('row'), lax.axis_index('col')
    tiles = half // TM
    kept = k0 >= half - KEEP
    if final:
        keep, (out, ov, osem) = rest[0], rest[-3:]
    elif kept:
        keep, out = rest
    else:
        l_refs, (out, bv, lv, lsem, bsem) = rest[:4], rest[4:]
    which = lax.bitwise_xor(k0 // depth, col)

    def l_copy(ref, t):
        slot = lax.rem(t, 2)
        return pltpu.make_async_copy(
            ref.at[pl.ds(t * TM, TM), pl.ds(k0 % depth, kw)], lv.at[slot], lsem.at[slot])

    def l_start(t):
        for i, ref in enumerate(l_refs):
            @pl.when(which == i)
            def _():
                l_copy(ref, t).start()

    def o_copy(t):
        return pltpu.make_async_copy(
            ov.at[t], out.at[pl.ds(t * TM, TM), pl.ds(dst0, width)], osem.at[t])

    def put(t, rows, total):
        if final:
            ov[t] = total.astype(ov.dtype)
            o_copy(t).start()
        else:
            out[rows, pl.ds(src0, width)] = total

    @pl.when(row == 1)
    def _():
        if not kept:
            b_copy = pltpu.make_async_copy(piece, bv, bsem)
            b_copy.start()
            l_start(0)
            l_start(1)
            b_copy.wait()
        right = piece if kept else bv

        def add(t, _):
            rows = pl.ds(pl.multiple_of(t * TM, TM), TM)
            if kept:
                tile = keep[rows, pl.ds(k0 - (half - KEEP), kw)]
            else:
                l_copy(l_refs[0], t).wait()
                tile = lv[lax.rem(t, 2)]
            put(t, rows, part[rows, pl.ds(src0, width)] + DOT(tile, right[...]))
            if not kept:
                @pl.when(t + 2 < tiles)
                def _():
                    l_start(t + 2)
            return 0

        lax.fori_loop(0, tiles, add, 0, unroll=kept)

    @pl.when(row == 0)
    def _():
        def move(t, _):
            rows = pl.ds(pl.multiple_of(t * TM, TM), TM)
            put(t, rows, part[rows, pl.ds(src0, width)])
            return 0

        lax.fori_loop(0, tiles, move, 0)

    if final:
        for t in range(tiles):
            o_copy(t).wait()


def solution(mesh):
    block_spec = P(('batch', 'row'), 'col')
    x_swap = [(0, 2), (1, 3), (2, 0), (3, 1)]
    core_swap = [(0, 1), (1, 0), (2, 3), (3, 2)]
    n_first = len(FIRST) + 1
    hbm = pl.BlockSpec(memory_space=pltpu.HBM)
    vmem = pl.BlockSpec(memory_space=pltpu.VMEM)
    smem = pl.BlockSpec(memory_space=pltpu.SMEM)

    def in_hbm(array):
        return pltpu.with_memory_space_constraint(array, pltpu.HBM)

    def product(l_block, b_block):
        half, depth = l_block.shape
        dtype = b_block.dtype
        off_counts, off_tab = plan(half, True)
        diag_counts, diag_tab = plan(half, False)
        info = jnp.stack([lax.axis_index('row'), lax.axis_index('col')]).astype(jnp.int32)
        starts = np.cumsum((0,) + WIDTHS).tolist()
        tail0, tail_w = starts[-1], b_block.shape[1] - starts[-1]

        cuts0 = np.cumsum((0,) + FIRST).tolist()
        boxes = [(r, e - r, 0, WIDTHS[0]) for r, e in zip(cuts0, cuts0[1:] + [half])]
        boxes += [(0, half, c, w) for c, w in zip(starts[1:], WIDTHS[1:])]
        n_main = len(boxes)
        ends = np.cumsum(TAIL).tolist()
        boxes += [(e - h, h, tail0, tail_w) for e, h in zip(ends[:-1], TAIL)]
        n_early, c = len(boxes) - 1, tail0
        for w, ks in LAST:
            boxes += [(half - TAIL[-1] + e - h, h, c, w) for e, h in zip(np.cumsum(ks).tolist(), ks)]
            c += w
        recv, source = [], b_block

        def send(j, source):
            r, h, c, w = boxes[j]
            piece = source[r:r + h, c:c + w]
            piece, source = lax.optimization_barrier((piece, source))
            recv.append(lax.ppermute(piece, 'row', [(0, 1), (1, 0)] if j == 0 else [(0, 1)]))
            return source

        for j in range(n_early):
            source = send(j, source)
        lx = lax.ppermute(l_block, 'col', x_swap)
        lc = lax.ppermute(l_block, 'col', core_swap)
        lxc = lax.ppermute(lx, 'col', core_swap)
        l_refs = [l_block, lc, lx, lxc]

        def chunk(pieces, cuts, x, src0, dst0, width, counts, tab):
            alias = [] if x is None else [x]
            operands = [tab, info, *map(in_hbm, [*l_refs, b_block, *pieces]), *alias]
            scratch = [
                pltpu.VMEM(((2 if cuts else 1) * half, width), dtype),
                pltpu.VMEM((NBUF, TM, KB), dtype),
                pltpu.VMEM((TM, width), jnp.float32),
            ]
            sems = [pltpu.SemaphoreType.DMA((NBUF,)), pltpu.SemaphoreType.DMA((2 * half // KB,))]
            if cuts:
                out, out_spec = jax.ShapeDtypeStruct(b_block.shape, dtype), hbm
                scratch += [pltpu.VMEM((2, TM, width), dtype), *sems, pltpu.SemaphoreType.DMA((2,))]
            else:
                out = (pltpu.VMEM((half, width), jnp.float32), pltpu.VMEM((half, KEEP), dtype))
                out_spec = (vmem, vmem)
                scratch += [*sems, pltpu.SemaphoreType.DMA]
            limit = 2 * (NBUF * TM * KB + (2 if cuts else 1) * half * width + 6 * TM * width) + 2 * 2**20
            return pl.pallas_call(
                functools.partial(chunk_kernel, half, depth, src0, dst0, width, counts, cuts, len(alias)),
                out_shape=out,
                in_specs=[smem, smem] + [hbm] * (len(operands) - 2), out_specs=out_spec,
                scratch_shapes=scratch,
                input_output_aliases={len(operands) - 1: 0} if alias else {},
                compiler_params=pltpu.CompilerParams(vmem_limit_bytes=limit),
                cost_estimate=pl.CostEstimate(flops=max(counts) * 2 * TM * KB * width,
                                              bytes_accessed=max(counts) * 2 * TM * KB, transcendentals=0),
            )(*operands)

        def tail(keep, piece, part, x, k0, kw, src0, width):
            final, kept = x is not None, k0 >= half - KEEP
            operands = [part, pltpu.with_memory_space_constraint(piece, pltpu.VMEM) if kept else in_hbm(piece)]
            operands += [keep] if kept else list(map(in_hbm, l_refs))
            specs = [vmem] + ([vmem, vmem] if kept else [hbm] * 5)
            scratch, need = [], 4 * TM * width + 2 * 2**20
            if final:
                operands.append(x)
                specs.append(hbm)
                out, out_spec = jax.ShapeDtypeStruct(x.shape, x.dtype), hbm
                scratch = [pltpu.VMEM((half // TM, TM, width), dtype), pltpu.SemaphoreType.DMA((half // TM,))]
                need += 2 * half * width
            else:
                out, out_spec = pltpu.VMEM(part.shape, part.dtype), vmem
                if not kept:
                    scratch = [pltpu.VMEM((kw, width), dtype), pltpu.VMEM((2, TM, kw), dtype),
                               pltpu.SemaphoreType.DMA((2,)), pltpu.SemaphoreType.DMA]
                    need += 2 * kw * (width + 2 * TM)
            return pl.pallas_call(
                functools.partial(tail_kernel, half, depth, k0, kw, src0, tail0 + src0, width, final),
                out_shape=out,
                in_specs=specs, out_specs=out_spec,
                scratch_shapes=scratch,
                input_output_aliases={len(operands) - 1: 0} if final else {0: 0},
                compiler_params=pltpu.CompilerParams(vmem_limit_bytes=need),
                cost_estimate=pl.CostEstimate(flops=2 * half * kw * width,
                                              bytes_accessed=2 * half * kw, transcendentals=0),
            )(*operands)

        x, part = None, None
        for j, width in enumerate(WIDTHS):
            if j == len(WIDTHS) - 1:
                x, b_block = lax.optimization_barrier((x, b_block))
                source = b_block
                for i in range(n_early, len(boxes)):
                    source = send(i, source)
                part, keep = chunk([], (), None, tail0, 0, tail_w, diag_counts, diag_tab)
                x, part, keep = lax.optimization_barrier((x, part, keep))
            pieces, cuts = (recv[:n_first], tuple(cuts0)) if j == 0 else ([recv[n_first - 1 + j]], (0,))
            x = chunk(pieces, cuts, x, starts[j], starts[j], width, off_counts, off_tab)
        x, part = lax.optimization_barrier((x, part))
        for piece, (k0, kw, c, w) in zip(recv[n_main:], boxes[n_main:]):
            final = k0 + kw == half
            done = tail(keep, piece, part, x if final else None, k0, kw, c - tail0, w)
            part, x = (part, done) if final else (done, x)
            x, part = lax.optimization_barrier((x, part))
        return x

    return jax.shard_map(product, mesh=mesh, in_specs=(block_spec, block_spec), out_specs=block_spec, check_vma=False)
```

```python
import functools

import jax
import jax.numpy as jnp
import numpy as np
from jax import lax
from jax.experimental import pallas as pl
from jax.experimental.pallas import tpu as pltpu
from jax.sharding import PartitionSpec as P


TM = 1024
KB = 1024
NBUF = 6
FIELDS = 6
WIDTHS = (512, 1024, 1024, 512, 512)
FIRST = (384, 640)
TAIL = (2048, 1024, 512, 512)
LAST = ((256, (512,)), (256, (256, 256)))
KEEP = 1024
DOT = functools.partial(jnp.dot, preferred_element_type=jnp.float32)


def plan(half, with_off):
    tables, nb = [], half // KB
    for row in range(2):
        start = row * nb
        steps, seen = [], set()
        for r in range(half // TM):
            ks = list(range(0 if with_off else start, start + -(-(r + 1) * TM // KB)))
            for k in ks:
                slot = k if with_off else k - start
                steps.append((r, k, int(k == ks[0]), int(k == ks[-1]), int(k not in seen), slot))
                seen.add(k)
        tables.append(steps)
    counts = tuple(len(s) for s in tables)
    flat = np.zeros((2, max(counts), FIELDS), np.int32)
    for row in range(2):
        flat[row, :counts[row]] = tables[row]
    return counts, jnp.asarray(flat.reshape(-1))


def chunk_kernel(half, depth, src0, dst0, width, counts, cuts, n_alias, tab, info, l0, l1, l2, l3, b_loc, *rest):
    pieces = rest[:len(cuts)]
    rest = rest[len(cuts) + n_alias:]
    off = bool(cuts)
    if off:
        out, bv, lv, acc, ov, lsem, bsem, osem = rest
    else:
        out, keep, bv, lv, acc, lsem, bsem, ksem = rest
    row, col = info[0], info[1]
    stride = max(counts) * FIELDS
    n = jnp.where(row == 0, counts[0], counts[1])
    per, nb = depth // KB, half // KB

    def field(t, f):
        return tab[row * stride + t * FIELDS + f]

    def l_start(t, slot):
        r, k = field(t, 0), field(t, 1)
        which = lax.bitwise_xor(k // per, col)
        for i, ref in enumerate((l0, l1, l2, l3)):
            @pl.when(which == i)
            def _():
                pltpu.make_async_copy(
                    ref.at[pl.ds(r * TM, TM), pl.ds(lax.rem(k, per) * KB, KB)],
                    lv.at[slot], lsem.at[slot]).start()

    def b_local(k, slot):
        return pltpu.make_async_copy(
            b_loc.at[pl.ds(k * KB, KB), pl.ds(src0, width)], bv.at[pl.ds(slot * KB, KB), :], bsem.at[slot])

    def b_recv_start(k):
        for ref, cut in zip(pieces, cuts):
            lo, hi = max(k * KB, cut), min((k + 1) * KB, cut + ref.shape[0])
            if lo < hi:
                pltpu.make_async_copy(
                    ref.at[pl.ds(lo - cut, hi - lo), :], bv.at[pl.ds(lo, hi - lo), :], bsem.at[k]).start()

    def o_copy(r, slot):
        return pltpu.make_async_copy(
            ov.at[slot], out.at[pl.ds(r * TM, TM), pl.ds(dst0, width)], osem.at[slot])

    def keep_copy(ref):
        return pltpu.make_async_copy(ref.at[:, pl.ds((half - KEEP) % depth, KEEP)], keep, ksem)

    for k in range(nb):
        if off:
            @pl.when(row == 0)
            def _():
                b_local(k, k).start()

            @pl.when(row == 1)
            def _():
                b_recv_start(k)
        else:
            b_local(k, k).start()
        l_start(k, k)
    if off:
        for k in range(nb):
            @pl.when(row == 1)
            def _():
                b_local(k, nb + k).start()
    for t in range(nb, NBUF - 1):
        l_start(t, t)
    if not off:
        kept = lax.bitwise_xor((half - KEEP) // depth, col)
        for i, ref in enumerate((l0, l1, l2, l3)):
            @pl.when((row == 1) & (kept == i))
            def _():
                keep_copy(ref).start()

    def step(t, _):
        slot = lax.rem(t, NBUF)
        r, at = field(t, 0), field(t, 5)

        @pl.when(t + NBUF - 1 < n)
        def _():
            l_start(t + NBUF - 1, lax.rem(t + NBUF - 1, NBUF))

        @pl.when(field(t, 4) == 1)
        def _():
            b_local(0, at).wait()

        pltpu.make_async_copy(l0.at[pl.ds(0, TM), pl.ds(0, KB)], lv.at[slot], lsem.at[slot]).wait()
        rows_k = pl.ds(pl.multiple_of(at * KB, KB), KB)
        first = field(t, 2)

        @pl.when(first == 1)
        def _():
            acc[...] = DOT(lv[slot], bv[rows_k, :])

        @pl.when(first == 0)
        def _():
            acc[...] += DOT(lv[slot], bv[rows_k, :])

        @pl.when(field(t, 3) == 1)
        def _():
            if off:
                oslot = lax.rem(r, 2)

                @pl.when(r >= 2)
                def _():
                    o_copy(r - 2, oslot).wait()

                ov[oslot] = acc[...].astype(ov.dtype)
                o_copy(r, oslot).start()
            else:
                out[pl.ds(pl.multiple_of(r * TM, TM), TM), :] = acc[...]

        return 0

    lax.fori_loop(0, n, step, 0)
    if off:
        last = half // TM
        o_copy(last - 2, (last - 2) % 2).wait()
        o_copy(last - 1, (last - 1) % 2).wait()
    else:
        @pl.when(row == 1)
        def _():
            keep_copy(l0).wait()


def tail_kernel(half, depth, k0, kw, src0, dst0, width, final, early, part, piece, *rest):
    row, col = lax.axis_index('row'), lax.axis_index('col')
    tiles = half // TM
    kept = k0 >= half - KEEP
    if final:
        keep, (out, ov, osem) = rest[0], rest[-3:]
    elif kept:
        keep, out = rest
    else:
        l_refs, (out, bv, lv, lsem, bsem) = rest[:4], rest[4:]
    which = lax.bitwise_xor(k0 // depth, col)

    def l_copy(ref, t):
        slot = lax.rem(t, 2)
        return pltpu.make_async_copy(
            ref.at[pl.ds(t * TM, TM), pl.ds(k0 % depth, kw)], lv.at[slot], lsem.at[slot])

    def l_start(t):
        for i, ref in enumerate(l_refs):
            @pl.when(which == i)
            def _():
                l_copy(ref, t).start()

    def o_copy(t, c=src0):
        return pltpu.make_async_copy(
            ov.at[t], out.at[pl.ds(t * TM, TM), pl.ds(dst0 + c, width)], osem.at[t])

    def put(t, rows, total):
        if final:
            ov[t] = total.astype(ov.dtype)
            o_copy(t).start()
        else:
            out[rows, pl.ds(src0, width)] = total

    @pl.when(row == 1)
    def _():
        if not kept:
            b_copy = pltpu.make_async_copy(piece, bv, bsem)
            b_copy.start()
            l_start(0)
            l_start(1)
            b_copy.wait()
        right = piece if kept else bv

        def add(t, _):
            rows = pl.ds(pl.multiple_of(t * TM, TM), TM)
            if kept:
                tile = keep[rows, pl.ds(k0 - (half - KEEP), kw)]
            else:
                l_copy(l_refs[0], t).wait()
                tile = lv[lax.rem(t, 2)]
            put(t, rows, part[rows, pl.ds(src0, width)] + DOT(tile, right[...]))
            if not kept:
                @pl.when(t + 2 < tiles)
                def _():
                    l_start(t + 2)
            return 0

        lax.fori_loop(0, tiles, add, 0, unroll=kept)

    if final:
        @pl.when(row == 1)
        def _():
            for t in range(tiles):
                o_copy(t).wait()

    if early:
        @pl.when(row == 0)
        def _():
            for c in range(0, part.shape[1], width):
                def move(t, _):
                    rows = pl.ds(pl.multiple_of(t * TM, TM), TM)
                    ov[t] = part[rows, pl.ds(c, width)].astype(ov.dtype)
                    o_copy(t, c).start()
                    return 0

                lax.fori_loop(0, tiles, move, 0)
                for t in range(tiles):
                    o_copy(t, c).wait()


def solution(mesh):
    block_spec = P(('batch', 'row'), 'col')
    x_swap = [(0, 2), (1, 3), (2, 0), (3, 1)]
    core_swap = [(0, 1), (1, 0), (2, 3), (3, 2)]
    n_first = len(FIRST) + 1
    hbm = pl.BlockSpec(memory_space=pltpu.HBM)
    vmem = pl.BlockSpec(memory_space=pltpu.VMEM)
    smem = pl.BlockSpec(memory_space=pltpu.SMEM)

    def in_hbm(array):
        return pltpu.with_memory_space_constraint(array, pltpu.HBM)

    def product(l_block, b_block):
        half, depth = l_block.shape
        dtype = b_block.dtype
        off_counts, off_tab = plan(half, True)
        diag_counts, diag_tab = plan(half, False)
        info = jnp.stack([lax.axis_index('row'), lax.axis_index('col')]).astype(jnp.int32)
        starts = np.cumsum((0,) + WIDTHS).tolist()
        tail0, tail_w = starts[-1], b_block.shape[1] - starts[-1]

        cuts0 = np.cumsum((0,) + FIRST).tolist()
        boxes = [(r, e - r, 0, WIDTHS[0]) for r, e in zip(cuts0, cuts0[1:] + [half])]
        boxes += [(0, half, c, w) for c, w in zip(starts[1:], WIDTHS[1:])]
        n_main = len(boxes)
        ends = np.cumsum(TAIL).tolist()
        boxes += [(e - h, h, tail0, tail_w) for e, h in zip(ends[:-1], TAIL)]
        n_early, c = len(boxes) - 1, tail0
        for w, ks in LAST:
            boxes += [(half - TAIL[-1] + e - h, h, c, w) for e, h in zip(np.cumsum(ks).tolist(), ks)]
            c += w
        recv, source = [], b_block

        def send(j, source):
            r, h, c, w = boxes[j]
            piece = source[r:r + h, c:c + w]
            piece, source = lax.optimization_barrier((piece, source))
            recv.append(lax.ppermute(piece, 'row', [(0, 1), (1, 0)] if j == 0 else [(0, 1)]))
            return source

        for j in range(n_early):
            source = send(j, source)
        lx = lax.ppermute(l_block, 'col', x_swap)
        lc = lax.ppermute(l_block, 'col', core_swap)
        lxc = lax.ppermute(lx, 'col', core_swap)
        l_refs = [l_block, lc, lx, lxc]

        def chunk(pieces, cuts, x, src0, dst0, width, counts, tab):
            alias = [] if x is None else [x]
            operands = [tab, info, *map(in_hbm, [*l_refs, b_block, *pieces]), *alias]
            scratch = [
                pltpu.VMEM(((2 if cuts else 1) * half, width), dtype),
                pltpu.VMEM((NBUF, TM, KB), dtype),
                pltpu.VMEM((TM, width), jnp.float32),
            ]
            sems = [pltpu.SemaphoreType.DMA((NBUF,)), pltpu.SemaphoreType.DMA((2 * half // KB,))]
            if cuts:
                out, out_spec = jax.ShapeDtypeStruct(b_block.shape, dtype), hbm
                scratch += [pltpu.VMEM((2, TM, width), dtype), *sems, pltpu.SemaphoreType.DMA((2,))]
            else:
                out = (pltpu.VMEM((half, width), jnp.float32), pltpu.VMEM((half, KEEP), dtype))
                out_spec = (vmem, vmem)
                scratch += [*sems, pltpu.SemaphoreType.DMA]
            limit = 2 * (NBUF * TM * KB + (2 if cuts else 1) * half * width + 6 * TM * width) + 2 * 2**20
            return pl.pallas_call(
                functools.partial(chunk_kernel, half, depth, src0, dst0, width, counts, cuts, len(alias)),
                out_shape=out,
                in_specs=[smem, smem] + [hbm] * (len(operands) - 2), out_specs=out_spec,
                scratch_shapes=scratch,
                input_output_aliases={len(operands) - 1: 0} if alias else {},
                compiler_params=pltpu.CompilerParams(vmem_limit_bytes=limit),
                cost_estimate=pl.CostEstimate(flops=max(counts) * 2 * TM * KB * width,
                                              bytes_accessed=max(counts) * 2 * TM * KB, transcendentals=0),
            )(*operands)

        def tail(keep, piece, part, x, k0, kw, src0, width):
            final, kept = x is not None, k0 >= half - KEEP
            operands = [part, pltpu.with_memory_space_constraint(piece, pltpu.VMEM) if kept else in_hbm(piece)]
            operands += [keep] if kept else list(map(in_hbm, l_refs))
            specs = [vmem] + ([vmem, vmem] if kept else [hbm] * 5)
            scratch, need = [], 4 * TM * width + 2 * 2**20
            if final:
                operands.append(x)
                specs.append(hbm)
                out, out_spec = jax.ShapeDtypeStruct(x.shape, x.dtype), hbm
                scratch = [pltpu.VMEM((half // TM, TM, width), dtype), pltpu.SemaphoreType.DMA((half // TM,))]
                need += 2 * half * width
            else:
                out, out_spec = pltpu.VMEM(part.shape, part.dtype), vmem
                if not kept:
                    scratch = [pltpu.VMEM((kw, width), dtype), pltpu.VMEM((2, TM, kw), dtype),
                               pltpu.SemaphoreType.DMA((2,)), pltpu.SemaphoreType.DMA]
                    need += 2 * kw * (width + 2 * TM)
            return pl.pallas_call(
                functools.partial(tail_kernel, half, depth, k0, kw, src0, tail0, width, final, final and src0 == 0),
                out_shape=out,
                in_specs=specs, out_specs=out_spec,
                scratch_shapes=scratch,
                input_output_aliases={len(operands) - 1: 0} if final else {0: 0},
                compiler_params=pltpu.CompilerParams(vmem_limit_bytes=need),
                cost_estimate=pl.CostEstimate(flops=2 * half * kw * width,
                                              bytes_accessed=2 * half * kw, transcendentals=0),
            )(*operands)

        x, part = None, None
        for j, width in enumerate(WIDTHS):
            if j == len(WIDTHS) - 1:
                x, b_block = lax.optimization_barrier((x, b_block))
                source = b_block
                for i in range(n_early, len(boxes)):
                    source = send(i, source)
                part, keep = chunk([], (), None, tail0, 0, tail_w, diag_counts, diag_tab)
                x, part, keep = lax.optimization_barrier((x, part, keep))
            pieces, cuts = (recv[:n_first], tuple(cuts0)) if j == 0 else ([recv[n_first - 1 + j]], (0,))
            x = chunk(pieces, cuts, x, starts[j], starts[j], width, off_counts, off_tab)
        x, part = lax.optimization_barrier((x, part))
        for piece, (k0, kw, c, w) in zip(recv[n_main:], boxes[n_main:]):
            final = k0 + kw == half
            done = tail(keep, piece, part, x if final else None, k0, kw, c - tail0, w)
            part, x = (part, done) if final else (done, x)
            x, part = lax.optimization_barrier((x, part))
        return x

    return jax.shard_map(product, mesh=mesh, in_specs=(block_spec, block_spec), out_specs=block_spec, check_vma=False)
```

```python
import functools

import jax
import jax.numpy as jnp
import numpy as np
from jax import lax
from jax.experimental import pallas as pl
from jax.experimental.pallas import tpu as pltpu
from jax.sharding import PartitionSpec as P


TM = 1024
KB = 1024
NBUF = 6
FIELDS = 6
WIDTHS = (512, 1024, 1024, 512, 512)
FIRST = (288, 736)
TAIL = (2048, 1024, 512, 512)
LAST = ((256, (512,)), (256, (256, 256)))
KEEP = 1024
DOT = functools.partial(jnp.dot, preferred_element_type=jnp.float32)


def plan(half, with_off):
    tables, nb = [], half // KB
    for row in range(2):
        start = row * nb
        steps, seen = [], set()
        for r in range(half // TM):
            ks = list(range(0 if with_off else start, start + -(-(r + 1) * TM // KB)))
            for k in ks:
                slot = k if with_off else k - start
                steps.append((r, k, int(k == ks[0]), int(k == ks[-1]), int(k not in seen), slot))
                seen.add(k)
        tables.append(steps)
    counts = tuple(len(s) for s in tables)
    flat = np.zeros((2, max(counts), FIELDS), np.int32)
    for row in range(2):
        flat[row, :counts[row]] = tables[row]
    return counts, jnp.asarray(flat.reshape(-1))


def chunk_kernel(half, depth, src0, dst0, width, counts, cuts, n_alias, tab, info, l0, l1, l2, l3, b_loc, *rest):
    pieces = rest[:len(cuts)]
    rest = rest[len(cuts) + n_alias:]
    off = bool(cuts)
    if off:
        out, bv, lv, acc, ov, lsem, bsem, osem = rest
    else:
        out, keep, bv, lv, acc, lsem, bsem, ksem = rest
    row, col = info[0], info[1]
    stride = max(counts) * FIELDS
    n = jnp.where(row == 0, counts[0], counts[1])
    per, nb = depth // KB, half // KB

    def field(t, f):
        return tab[row * stride + t * FIELDS + f]

    def l_start(t, slot):
        r, k = field(t, 0), field(t, 1)
        which = lax.bitwise_xor(k // per, col)
        for i, ref in enumerate((l0, l1, l2, l3)):
            @pl.when(which == i)
            def _():
                pltpu.make_async_copy(
                    ref.at[pl.ds(r * TM, TM), pl.ds(lax.rem(k, per) * KB, KB)],
                    lv.at[slot], lsem.at[slot]).start()

    def b_local(k, slot):
        return pltpu.make_async_copy(
            b_loc.at[pl.ds(k * KB, KB), pl.ds(src0, width)], bv.at[pl.ds(slot * KB, KB), :], bsem.at[slot])

    def b_recv_start(k):
        for i, (ref, cut) in enumerate(zip(pieces, cuts)):
            lo, hi = max(k * KB, cut), min((k + 1) * KB, cut + ref.shape[0])
            if lo < hi:
                @pl.when(lax.rem(col, 2) == i - cuts.index(cut) if cuts.count(cut) > 1 else True)
                def _():
                    pltpu.make_async_copy(
                        ref.at[pl.ds(lo - cut, hi - lo), :], bv.at[pl.ds(lo, hi - lo), :], bsem.at[k]).start()

    def o_copy(r, slot):
        return pltpu.make_async_copy(
            ov.at[slot], out.at[pl.ds(r * TM, TM), pl.ds(dst0, width)], osem.at[slot])

    def keep_copy(ref):
        return pltpu.make_async_copy(ref.at[:, pl.ds((half - KEEP) % depth, KEEP)], keep, ksem)

    for k in range(nb):
        if off:
            @pl.when(row == 0)
            def _():
                b_local(k, k).start()

            @pl.when(row == 1)
            def _():
                b_recv_start(k)
        else:
            b_local(k, k).start()
        l_start(k, k)
    if off:
        for k in range(nb):
            @pl.when(row == 1)
            def _():
                b_local(k, nb + k).start()
    for t in range(nb, NBUF - 1):
        l_start(t, t)
    if not off:
        kept = lax.bitwise_xor((half - KEEP) // depth, col)
        for i, ref in enumerate((l0, l1, l2, l3)):
            @pl.when((row == 1) & (kept == i))
            def _():
                keep_copy(ref).start()

    def step(t, _):
        slot = lax.rem(t, NBUF)
        r, at = field(t, 0), field(t, 5)

        @pl.when(t + NBUF - 1 < n)
        def _():
            l_start(t + NBUF - 1, lax.rem(t + NBUF - 1, NBUF))

        @pl.when(field(t, 4) == 1)
        def _():
            b_local(0, at).wait()

        pltpu.make_async_copy(l0.at[pl.ds(0, TM), pl.ds(0, KB)], lv.at[slot], lsem.at[slot]).wait()
        rows_k = pl.ds(pl.multiple_of(at * KB, KB), KB)
        first = field(t, 2)

        @pl.when(first == 1)
        def _():
            acc[...] = DOT(lv[slot], bv[rows_k, :])

        @pl.when(first == 0)
        def _():
            acc[...] += DOT(lv[slot], bv[rows_k, :])

        @pl.when(field(t, 3) == 1)
        def _():
            if off:
                oslot = lax.rem(r, 2)

                @pl.when(r >= 2)
                def _():
                    o_copy(r - 2, oslot).wait()

                ov[oslot] = acc[...].astype(ov.dtype)
                o_copy(r, oslot).start()
            else:
                out[pl.ds(pl.multiple_of(r * TM, TM), TM), :] = acc[...]

        return 0

    lax.fori_loop(0, n, step, 0)
    if off:
        last = half // TM
        o_copy(last - 2, (last - 2) % 2).wait()
        o_copy(last - 1, (last - 1) % 2).wait()
    else:
        @pl.when(row == 1)
        def _():
            keep_copy(l0).wait()


def tail_kernel(half, depth, k0, kw, src0, dst0, width, final, early, part, piece, *rest):
    row, col = lax.axis_index('row'), lax.axis_index('col')
    tiles = half // TM
    kept = k0 >= half - KEEP
    if final:
        keep, (out, ov, osem) = rest[0], rest[-3:]
    elif kept:
        keep, out = rest
    else:
        l_refs, (out, bv, lv, lsem, bsem) = rest[:4], rest[4:]
    which = lax.bitwise_xor(k0 // depth, col)

    def l_copy(ref, t):
        slot = lax.rem(t, 2)
        return pltpu.make_async_copy(
            ref.at[pl.ds(t * TM, TM), pl.ds(k0 % depth, kw)], lv.at[slot], lsem.at[slot])

    def l_start(t):
        for i, ref in enumerate(l_refs):
            @pl.when(which == i)
            def _():
                l_copy(ref, t).start()

    def o_copy(t, c=src0):
        return pltpu.make_async_copy(
            ov.at[t], out.at[pl.ds(t * TM, TM), pl.ds(dst0 + c, width)], osem.at[t])

    def put(t, rows, total):
        if final:
            ov[t] = total.astype(ov.dtype)
            o_copy(t).start()
        else:
            out[rows, pl.ds(src0, width)] = total

    @pl.when(row == 1)
    def _():
        if not kept:
            b_copy = pltpu.make_async_copy(piece, bv, bsem)
            b_copy.start()
            l_start(0)
            l_start(1)
            b_copy.wait()
        right = piece if kept else bv

        def add(t, _):
            rows = pl.ds(pl.multiple_of(t * TM, TM), TM)
            if kept:
                tile = keep[rows, pl.ds(k0 - (half - KEEP), kw)]
            else:
                l_copy(l_refs[0], t).wait()
                tile = lv[lax.rem(t, 2)]
            put(t, rows, part[rows, pl.ds(src0, width)] + DOT(tile, right[...]))
            if not kept:
                @pl.when(t + 2 < tiles)
                def _():
                    l_start(t + 2)
            return 0

        lax.fori_loop(0, tiles, add, 0, unroll=kept)

    if final:
        @pl.when(row == 1)
        def _():
            for t in range(tiles):
                o_copy(t).wait()

    if early:
        @pl.when(row == 0)
        def _():
            for c in range(0, part.shape[1], width):
                def move(t, _):
                    rows = pl.ds(pl.multiple_of(t * TM, TM), TM)
                    ov[t] = part[rows, pl.ds(c, width)].astype(ov.dtype)
                    o_copy(t, c).start()
                    return 0

                lax.fori_loop(0, tiles, move, 0)
                for t in range(tiles):
                    o_copy(t, c).wait()


def solution(mesh):
    block_spec = P(('batch', 'row'), 'col')
    x_swap = [(0, 2), (1, 3), (2, 0), (3, 1)]
    core_swap = [(0, 1), (1, 0), (2, 3), (3, 2)]
    n_first = len(FIRST) + 1
    n_cols = mesh.shape['col']
    hbm = pl.BlockSpec(memory_space=pltpu.HBM)
    vmem = pl.BlockSpec(memory_space=pltpu.VMEM)
    smem = pl.BlockSpec(memory_space=pltpu.SMEM)

    def in_hbm(array):
        return pltpu.with_memory_space_constraint(array, pltpu.HBM)

    def product(l_block, b_block):
        half, depth = l_block.shape
        dtype = b_block.dtype
        off_counts, off_tab = plan(half, True)
        diag_counts, diag_tab = plan(half, False)
        info = jnp.stack([lax.axis_index('row'), lax.axis_index('col')]).astype(jnp.int32)
        starts = np.cumsum((0,) + WIDTHS).tolist()
        tail0, tail_w = starts[-1], b_block.shape[1] - starts[-1]

        cuts0 = np.cumsum((0,) + FIRST).tolist()
        boxes = [(r, e - r, 0, WIDTHS[0]) for r, e in zip(cuts0, cuts0[1:] + [half])]
        boxes += [(0, half, c, w) for c, w in zip(starts[1:], WIDTHS[1:])]
        n_main = len(boxes)
        ends = np.cumsum(TAIL).tolist()
        boxes += [(e - h, h, tail0, tail_w) for e, h in zip(ends[:-1], TAIL)]
        n_early, c = len(boxes) - 1, tail0
        for w, ks in LAST:
            boxes += [(half - TAIL[-1] + e - h, h, c, w) for e, h in zip(np.cumsum(ks).tolist(), ks)]
            c += w
        recv, source = [], b_block

        def send(j, source):
            r, h, c, w = boxes[j]
            piece = source[r:r + h, c:c + w]
            piece, source = lax.optimization_barrier((piece, source))
            if j == 1:
                for core in range(2):
                    recv.append(lax.ppermute(piece, ('row', 'col'), [(c, c + n_cols) for c in range(core, n_cols, 2)]))
                return source
            recv.append(lax.ppermute(piece, 'row', [(0, 1), (1, 0)] if j == 0 else [(0, 1)]))
            return source

        for j in range(n_early):
            source = send(j, source)
        lx = lax.ppermute(l_block, 'col', x_swap)
        lc = lax.ppermute(l_block, 'col', core_swap)
        lxc = lax.ppermute(lx, 'col', core_swap)
        l_refs = [l_block, lc, lx, lxc]

        def chunk(pieces, cuts, x, src0, dst0, width, counts, tab):
            alias = [] if x is None else [x]
            operands = [tab, info, *map(in_hbm, [*l_refs, b_block, *pieces]), *alias]
            scratch = [
                pltpu.VMEM(((2 if cuts else 1) * half, width), dtype),
                pltpu.VMEM((NBUF, TM, KB), dtype),
                pltpu.VMEM((TM, width), jnp.float32),
            ]
            sems = [pltpu.SemaphoreType.DMA((NBUF,)), pltpu.SemaphoreType.DMA((2 * half // KB,))]
            if cuts:
                out, out_spec = jax.ShapeDtypeStruct(b_block.shape, dtype), hbm
                scratch += [pltpu.VMEM((2, TM, width), dtype), *sems, pltpu.SemaphoreType.DMA((2,))]
            else:
                out = (pltpu.VMEM((half, width), jnp.float32), pltpu.VMEM((half, KEEP), dtype))
                out_spec = (vmem, vmem)
                scratch += [*sems, pltpu.SemaphoreType.DMA]
            limit = 2 * (NBUF * TM * KB + (2 if cuts else 1) * half * width + 6 * TM * width) + 2 * 2**20
            return pl.pallas_call(
                functools.partial(chunk_kernel, half, depth, src0, dst0, width, counts, cuts, len(alias)),
                out_shape=out,
                in_specs=[smem, smem] + [hbm] * (len(operands) - 2), out_specs=out_spec,
                scratch_shapes=scratch,
                input_output_aliases={len(operands) - 1: 0} if alias else {},
                compiler_params=pltpu.CompilerParams(vmem_limit_bytes=limit),
                cost_estimate=pl.CostEstimate(flops=max(counts) * 2 * TM * KB * width,
                                              bytes_accessed=max(counts) * 2 * TM * KB, transcendentals=0),
            )(*operands)

        def tail(keep, piece, part, x, k0, kw, src0, width):
            final, kept = x is not None, k0 >= half - KEEP
            operands = [part, pltpu.with_memory_space_constraint(piece, pltpu.VMEM) if kept else in_hbm(piece)]
            operands += [keep] if kept else list(map(in_hbm, l_refs))
            specs = [vmem] + ([vmem, vmem] if kept else [hbm] * 5)
            scratch, need = [], 4 * TM * width + 2 * 2**20
            if final:
                operands.append(x)
                specs.append(hbm)
                out, out_spec = jax.ShapeDtypeStruct(x.shape, x.dtype), hbm
                scratch = [pltpu.VMEM((half // TM, TM, width), dtype), pltpu.SemaphoreType.DMA((half // TM,))]
                need += 2 * half * width
            else:
                out, out_spec = pltpu.VMEM(part.shape, part.dtype), vmem
                if not kept:
                    scratch = [pltpu.VMEM((kw, width), dtype), pltpu.VMEM((2, TM, kw), dtype),
                               pltpu.SemaphoreType.DMA((2,)), pltpu.SemaphoreType.DMA]
                    need += 2 * kw * (width + 2 * TM)
            return pl.pallas_call(
                functools.partial(tail_kernel, half, depth, k0, kw, src0, tail0, width, final, final and src0 == 0),
                out_shape=out,
                in_specs=specs, out_specs=out_spec,
                scratch_shapes=scratch,
                input_output_aliases={len(operands) - 1: 0} if final else {0: 0},
                compiler_params=pltpu.CompilerParams(vmem_limit_bytes=need),
                cost_estimate=pl.CostEstimate(flops=2 * half * kw * width,
                                              bytes_accessed=2 * half * kw, transcendentals=0),
            )(*operands)

        x, part = None, None
        for j, width in enumerate(WIDTHS):
            if j == len(WIDTHS) - 1:
                x, b_block = lax.optimization_barrier((x, b_block))
                source = b_block
                for i in range(n_early, len(boxes)):
                    source = send(i, source)
                part, keep = chunk([], (), None, tail0, 0, tail_w, diag_counts, diag_tab)
                x, part, keep = lax.optimization_barrier((x, part, keep))
            pieces, cuts = (recv[:n_first + 1], tuple(cuts0[:2] + cuts0[1:])) if j == 0 else ([recv[n_first + j]], (0,))
            x = chunk(pieces, cuts, x, starts[j], starts[j], width, off_counts, off_tab)
        x, part = lax.optimization_barrier((x, part))
        for piece, (k0, kw, c, w) in zip(recv[n_main + 1:], boxes[n_main:]):
            final = k0 + kw == half
            done = tail(keep, piece, part, x if final else None, k0, kw, c - tail0, w)
            part, x = (part, done) if final else (done, x)
            x, part = lax.optimization_barrier((x, part))
        return x

    return jax.shard_map(product, mesh=mesh, in_specs=(block_spec, block_spec), out_specs=block_spec, check_vma=False)
```

```python
import functools

import jax
import jax.numpy as jnp
import numpy as np
from jax import lax
from jax.experimental import pallas as pl
from jax.experimental.pallas import tpu as pltpu
from jax.sharding import PartitionSpec as P


TM = 1024
KB = 1024
NBUF = 6
FIELDS = 6
WIDTHS = (512, 1024, 1024, 512, 512)
FIRST = (288, 736)
TAIL = (2048, 1024, 512, 512)
LAST = ((256, (512,)), (256, (256, 256)))
KEEP = 1024
DOT = functools.partial(jnp.dot, preferred_element_type=jnp.float32)


def plan(half, with_off):
    tables, nb = [], half // KB
    for row in range(2):
        start = row * nb
        steps, seen = [], set()
        for r in range(half // TM):
            ks = list(range(0 if with_off else start, start + -(-(r + 1) * TM // KB)))
            for k in ks:
                slot = k if with_off else k - start
                steps.append((r, k, int(k == ks[0]), int(k == ks[-1]), int(k not in seen), slot))
                seen.add(k)
        tables.append(steps)
    counts = tuple(len(s) for s in tables)
    flat = np.zeros((2, max(counts), FIELDS), np.int32)
    for row in range(2):
        flat[row, :counts[row]] = tables[row]
    return counts, jnp.asarray(flat.reshape(-1))


def chunk_kernel(half, depth, src0, dst0, width, counts, cuts, n_alias, tab, info, l0, l1, l2, l3, b_loc, *rest):
    pieces = rest[:len(cuts)]
    rest = rest[len(cuts) + n_alias:]
    off = bool(cuts)
    if off:
        out, bv, lv, acc, ov, lsem, bsem, osem = rest
    else:
        out, keep, bv, lv, acc, lsem, bsem, ksem = rest
    row, col = info[0], info[1]
    stride = max(counts) * FIELDS
    n = jnp.where(row == 0, counts[0], counts[1])
    per, nb = depth // KB, half // KB

    def field(t, f):
        return tab[row * stride + t * FIELDS + f]

    def l_start(t, slot):
        r, k = field(t, 0), field(t, 1)
        which = lax.bitwise_xor(k // per, col)
        for i, ref in enumerate((l0, l1, l2, l3)):
            @pl.when(which == i)
            def _():
                pltpu.make_async_copy(
                    ref.at[pl.ds(r * TM, TM), pl.ds(lax.rem(k, per) * KB, KB)],
                    lv.at[slot], lsem.at[slot]).start()

    def b_local(k, slot):
        return pltpu.make_async_copy(
            b_loc.at[pl.ds(k * KB, KB), pl.ds(src0, width)], bv.at[pl.ds(slot * KB, KB), :], bsem.at[slot])

    def b_recv_start(k):
        for ref, cut in zip(pieces, cuts):
            lo, hi = max(k * KB, cut), min((k + 1) * KB, cut + ref.shape[0])
            if lo < hi:
                pltpu.make_async_copy(
                    ref.at[pl.ds(lo - cut, hi - lo), :], bv.at[pl.ds(lo, hi - lo), :], bsem.at[k]).start()

    def o_copy(r, slot):
        return pltpu.make_async_copy(
            ov.at[slot], out.at[pl.ds(r * TM, TM), pl.ds(dst0, width)], osem.at[slot])

    def keep_copy(ref):
        return pltpu.make_async_copy(ref.at[:, pl.ds((half - KEEP) % depth, KEEP)], keep, ksem)

    for k in range(nb):
        if off:
            @pl.when(row == 0)
            def _():
                b_local(k, k).start()

            @pl.when(row == 1)
            def _():
                b_recv_start(k)
        else:
            b_local(k, k).start()
        l_start(k, k)
    if off:
        for k in range(nb):
            @pl.when(row == 1)
            def _():
                b_local(k, nb + k).start()
    for t in range(nb, NBUF - 1):
        l_start(t, t)
    if not off:
        kept = lax.bitwise_xor((half - KEEP) // depth, col)
        for i, ref in enumerate((l0, l1, l2, l3)):
            @pl.when((row == 1) & (kept == i))
            def _():
                keep_copy(ref).start()

    def step(t, _):
        slot = lax.rem(t, NBUF)
        r, at = field(t, 0), field(t, 5)

        @pl.when(t + NBUF - 1 < n)
        def _():
            l_start(t + NBUF - 1, lax.rem(t + NBUF - 1, NBUF))

        @pl.when(field(t, 4) == 1)
        def _():
            b_local(0, at).wait()

        pltpu.make_async_copy(l0.at[pl.ds(0, TM), pl.ds(0, KB)], lv.at[slot], lsem.at[slot]).wait()
        rows_k = pl.ds(pl.multiple_of(at * KB, KB), KB)
        first = field(t, 2)

        @pl.when(first == 1)
        def _():
            acc[...] = DOT(lv[slot], bv[rows_k, :])

        @pl.when(first == 0)
        def _():
            acc[...] += DOT(lv[slot], bv[rows_k, :])

        @pl.when(field(t, 3) == 1)
        def _():
            if off:
                oslot = lax.rem(r, 2)

                @pl.when(r >= 2)
                def _():
                    o_copy(r - 2, oslot).wait()

                ov[oslot] = acc[...].astype(ov.dtype)
                o_copy(r, oslot).start()
            else:
                out[pl.ds(pl.multiple_of(r * TM, TM), TM), :] = acc[...]

        return 0

    lax.fori_loop(0, n, step, 0)
    if off:
        last = half // TM
        o_copy(last - 2, (last - 2) % 2).wait()
        o_copy(last - 1, (last - 1) % 2).wait()
    else:
        @pl.when(row == 1)
        def _():
            keep_copy(l0).wait()


def first_kernel(b_loc, out, sem):
    copy = pltpu.make_async_copy(b_loc.at[pl.ds(0, out.shape[0]), pl.ds(0, out.shape[1])], out, sem)

    @pl.when(lax.axis_index('row') == 0)
    def _():
        copy.start()
        copy.wait()


def tail_kernel(half, depth, k0, kw, src0, dst0, width, final, early, part, piece, *rest):
    row, col = lax.axis_index('row'), lax.axis_index('col')
    tiles = half // TM
    kept = k0 >= half - KEEP
    if final:
        keep, (out, ov, osem) = rest[0], rest[-3:]
    elif kept:
        keep, out = rest
    else:
        l_refs, (out, bv, lv, lsem, bsem) = rest[:4], rest[4:]
    which = lax.bitwise_xor(k0 // depth, col)

    def l_copy(ref, t):
        slot = lax.rem(t, 2)
        return pltpu.make_async_copy(
            ref.at[pl.ds(t * TM, TM), pl.ds(k0 % depth, kw)], lv.at[slot], lsem.at[slot])

    def l_start(t):
        for i, ref in enumerate(l_refs):
            @pl.when(which == i)
            def _():
                l_copy(ref, t).start()

    def o_copy(t, c=src0):
        return pltpu.make_async_copy(
            ov.at[t], out.at[pl.ds(t * TM, TM), pl.ds(dst0 + c, width)], osem.at[t])

    def put(t, rows, total):
        if final:
            ov[t] = total.astype(ov.dtype)
            o_copy(t).start()
        else:
            out[rows, pl.ds(src0, width)] = total

    @pl.when(row == 1)
    def _():
        if not kept:
            b_copy = pltpu.make_async_copy(piece, bv, bsem)
            b_copy.start()
            l_start(0)
            l_start(1)
            b_copy.wait()
        right = piece if kept else bv

        def add(t, _):
            rows = pl.ds(pl.multiple_of(t * TM, TM), TM)
            if kept:
                tile = keep[rows, pl.ds(k0 - (half - KEEP), kw)]
            else:
                l_copy(l_refs[0], t).wait()
                tile = lv[lax.rem(t, 2)]
            put(t, rows, part[rows, pl.ds(src0, width)] + DOT(tile, right[...]))
            if not kept:
                @pl.when(t + 2 < tiles)
                def _():
                    l_start(t + 2)
            return 0

        lax.fori_loop(0, tiles, add, 0, unroll=kept)

    if final:
        @pl.when(row == 1)
        def _():
            for t in range(tiles):
                o_copy(t).wait()

    if early:
        @pl.when(row == 0)
        def _():
            for c in range(0, part.shape[1], width):
                def move(t, _):
                    rows = pl.ds(pl.multiple_of(t * TM, TM), TM)
                    ov[t] = part[rows, pl.ds(c, width)].astype(ov.dtype)
                    o_copy(t, c).start()
                    return 0

                lax.fori_loop(0, tiles, move, 0)
                for t in range(tiles):
                    o_copy(t, c).wait()


def solution(mesh):
    block_spec = P(('batch', 'row'), 'col')
    x_swap = [(0, 2), (1, 3), (2, 0), (3, 1)]
    core_swap = [(0, 1), (1, 0), (2, 3), (3, 2)]
    n_first = len(FIRST) + 1
    hbm = pl.BlockSpec(memory_space=pltpu.HBM)
    vmem = pl.BlockSpec(memory_space=pltpu.VMEM)
    smem = pl.BlockSpec(memory_space=pltpu.SMEM)

    def in_hbm(array):
        return pltpu.with_memory_space_constraint(array, pltpu.HBM)

    def product(l_block, b_block):
        half, depth = l_block.shape
        dtype = b_block.dtype
        off_counts, off_tab = plan(half, True)
        diag_counts, diag_tab = plan(half, False)
        info = jnp.stack([lax.axis_index('row'), lax.axis_index('col')]).astype(jnp.int32)
        starts = np.cumsum((0,) + WIDTHS).tolist()
        tail0, tail_w = starts[-1], b_block.shape[1] - starts[-1]

        cuts0 = np.cumsum((0,) + FIRST).tolist()
        boxes = [(r, e - r, 0, WIDTHS[0]) for r, e in zip(cuts0, cuts0[1:] + [half])]
        boxes += [(0, half, c, w) for c, w in zip(starts[1:], WIDTHS[1:])]
        n_main = len(boxes)
        ends = np.cumsum(TAIL).tolist()
        boxes += [(e - h, h, tail0, tail_w) for e, h in zip(ends[:-1], TAIL)]
        n_early, c = len(boxes) - 1, tail0
        for w, ks in LAST:
            boxes += [(half - TAIL[-1] + e - h, h, c, w) for e, h in zip(np.cumsum(ks).tolist(), ks)]
            c += w
        recv, source = [], b_block

        def send(j, source):
            r, h, c, w = boxes[j]
            if j == 0:
                piece = pl.pallas_call(
                    first_kernel, out_shape=pltpu.VMEM((h, w), dtype), in_specs=[hbm], out_specs=vmem,
                    scratch_shapes=[pltpu.SemaphoreType.DMA],
                    compiler_params=pltpu.CompilerParams(vmem_limit_bytes=2**20), name="first",
                )(in_hbm(source))
            else:
                piece = source[r:r + h, c:c + w]
            piece, source = lax.optimization_barrier((piece, source))
            recv.append(lax.ppermute(piece, 'row', [(0, 1), (1, 0)] if j == 0 else [(0, 1)]))
            return source

        for j in range(n_early):
            source = send(j, source)
        lx = lax.ppermute(l_block, 'col', x_swap)
        lc = lax.ppermute(l_block, 'col', core_swap)
        lxc = lax.ppermute(lx, 'col', core_swap)
        l_refs = [l_block, lc, lx, lxc]

        def chunk(pieces, cuts, x, src0, dst0, width, counts, tab):
            alias = [] if x is None else [x]
            operands = [tab, info, *map(in_hbm, [*l_refs, b_block, *pieces]), *alias]
            scratch = [
                pltpu.VMEM(((2 if cuts else 1) * half, width), dtype),
                pltpu.VMEM((NBUF, TM, KB), dtype),
                pltpu.VMEM((TM, width), jnp.float32),
            ]
            sems = [pltpu.SemaphoreType.DMA((NBUF,)), pltpu.SemaphoreType.DMA((2 * half // KB,))]
            if cuts:
                out, out_spec = jax.ShapeDtypeStruct(b_block.shape, dtype), hbm
                scratch += [pltpu.VMEM((2, TM, width), dtype), *sems, pltpu.SemaphoreType.DMA((2,))]
            else:
                out = (pltpu.VMEM((half, width), jnp.float32), pltpu.VMEM((half, KEEP), dtype))
                out_spec = (vmem, vmem)
                scratch += [*sems, pltpu.SemaphoreType.DMA]
            limit = 2 * (NBUF * TM * KB + (2 if cuts else 1) * half * width + 6 * TM * width) + 2 * 2**20
            return pl.pallas_call(
                functools.partial(chunk_kernel, half, depth, src0, dst0, width, counts, cuts, len(alias)),
                out_shape=out,
                in_specs=[smem, smem] + [hbm] * (len(operands) - 2), out_specs=out_spec,
                scratch_shapes=scratch,
                input_output_aliases={len(operands) - 1: 0} if alias else {},
                compiler_params=pltpu.CompilerParams(vmem_limit_bytes=limit),
                cost_estimate=pl.CostEstimate(flops=max(counts) * 2 * TM * KB * width,
                                              bytes_accessed=max(counts) * 2 * TM * KB, transcendentals=0),
            )(*operands)

        def tail(keep, piece, part, x, k0, kw, src0, width):
            final, kept = x is not None, k0 >= half - KEEP
            operands = [part, pltpu.with_memory_space_constraint(piece, pltpu.VMEM) if kept else in_hbm(piece)]
            operands += [keep] if kept else list(map(in_hbm, l_refs))
            specs = [vmem] + ([vmem, vmem] if kept else [hbm] * 5)
            scratch, need = [], 4 * TM * width + 2 * 2**20
            if final:
                operands.append(x)
                specs.append(hbm)
                out, out_spec = jax.ShapeDtypeStruct(x.shape, x.dtype), hbm
                scratch = [pltpu.VMEM((half // TM, TM, width), dtype), pltpu.SemaphoreType.DMA((half // TM,))]
                need += 2 * half * width
            else:
                out, out_spec = pltpu.VMEM(part.shape, part.dtype), vmem
                if not kept:
                    scratch = [pltpu.VMEM((kw, width), dtype), pltpu.VMEM((2, TM, kw), dtype),
                               pltpu.SemaphoreType.DMA((2,)), pltpu.SemaphoreType.DMA]
                    need += 2 * kw * (width + 2 * TM)
            return pl.pallas_call(
                functools.partial(tail_kernel, half, depth, k0, kw, src0, tail0, width, final, final and src0 == 0),
                out_shape=out,
                in_specs=specs, out_specs=out_spec,
                scratch_shapes=scratch,
                input_output_aliases={len(operands) - 1: 0} if final else {0: 0},
                compiler_params=pltpu.CompilerParams(vmem_limit_bytes=need),
                cost_estimate=pl.CostEstimate(flops=2 * half * kw * width,
                                              bytes_accessed=2 * half * kw, transcendentals=0),
            )(*operands)

        x, part = None, None
        for j, width in enumerate(WIDTHS):
            if j == len(WIDTHS) - 1:
                x, b_block = lax.optimization_barrier((x, b_block))
                source = b_block
                for i in range(n_early, len(boxes)):
                    source = send(i, source)
                part, keep = chunk([], (), None, tail0, 0, tail_w, diag_counts, diag_tab)
                x, part, keep = lax.optimization_barrier((x, part, keep))
            pieces, cuts = (recv[:n_first], tuple(cuts0)) if j == 0 else ([recv[n_first - 1 + j]], (0,))
            x = chunk(pieces, cuts, x, starts[j], starts[j], width, off_counts, off_tab)
        x, part = lax.optimization_barrier((x, part))
        for piece, (k0, kw, c, w) in zip(recv[n_main:], boxes[n_main:]):
            final = k0 + kw == half
            done = tail(keep, piece, part, x if final else None, k0, kw, c - tail0, w)
            part, x = (part, done) if final else (done, x)
            x, part = lax.optimization_barrier((x, part))
        return x

    return jax.shard_map(product, mesh=mesh, in_specs=(block_spec, block_spec), out_specs=block_spec, check_vma=False)
```

```python
import functools

import jax
import jax.numpy as jnp
import numpy as np
from jax import lax
from jax.experimental import pallas as pl
from jax.experimental.pallas import tpu as pltpu
from jax.sharding import PartitionSpec as P


TM = 1024
KB = 1024
NBUF = 6
FIELDS = 6
WIDTHS = (512, 1024, 1024, 512, 512)
FIRST = (288, 736)
TAIL = (2048, 1024, 512, 512)
LAST = ((256, (512,)), (256, (256, 256)))
FINE = 512
KEEP = 1024
DOT = functools.partial(jnp.dot, preferred_element_type=jnp.float32)


def plan(half, with_off):
    tables, nb = [], half // KB
    for row in range(2):
        start = row * nb
        steps, seen = [], set()
        for r in range(half // TM):
            ks = list(range(0 if with_off else start, start + -(-(r + 1) * TM // KB)))
            for k in ks:
                slot = k if with_off else k - start
                steps.append((r, k, int(k == ks[0]), int(k == ks[-1]), int(k not in seen), slot))
                seen.add(k)
        tables.append(steps)
    counts = tuple(len(s) for s in tables)
    flat = np.zeros((2, max(counts), FIELDS), np.int32)
    for row in range(2):
        flat[row, :counts[row]] = tables[row]
    return counts, jnp.asarray(flat.reshape(-1))


def chunk_kernel(half, depth, src0, dst0, width, counts, cuts, n_alias, tab, info, l0, l1, l2, l3, b_loc, *rest):
    pieces = rest[:len(cuts)]
    rest = rest[len(cuts) + n_alias:]
    off = bool(cuts)
    if off:
        out, bv, lv, acc, ov, lsem, bsem, osem = rest
    else:
        out, keep, bv, lv, acc, lsem, bsem, ksem = rest
    row, col = info[0], info[1]
    stride = max(counts) * FIELDS
    n = jnp.where(row == 0, counts[0], counts[1])
    per, nb = depth // KB, half // KB

    def field(t, f):
        return tab[row * stride + t * FIELDS + f]

    def l_start(t, slot):
        r, k = field(t, 0), field(t, 1)
        which = lax.bitwise_xor(k // per, col)
        for i, ref in enumerate((l0, l1, l2, l3)):
            @pl.when(which == i)
            def _():
                pltpu.make_async_copy(
                    ref.at[pl.ds(r * TM, TM), pl.ds(lax.rem(k, per) * KB, KB)],
                    lv.at[slot], lsem.at[slot]).start()

    def b_local(k, slot):
        return pltpu.make_async_copy(
            b_loc.at[pl.ds(k * KB, KB), pl.ds(src0, width)], bv.at[pl.ds(slot * KB, KB), :], bsem.at[slot])

    def b_recv_start(k):
        for ref, cut in zip(pieces, cuts):
            lo, hi = max(k * KB, cut), min((k + 1) * KB, cut + ref.shape[0])
            if lo < hi:
                pltpu.make_async_copy(
                    ref.at[pl.ds(lo - cut, hi - lo), :], bv.at[pl.ds(lo, hi - lo), :], bsem.at[k]).start()

    def o_copy(r, slot):
        return pltpu.make_async_copy(
            ov.at[slot], out.at[pl.ds(r * TM, TM), pl.ds(dst0, width)], osem.at[slot])

    def keep_copy(ref):
        return pltpu.make_async_copy(ref.at[:, pl.ds((half - KEEP) % depth, KEEP)], keep, ksem)

    for k in range(nb):
        if off:
            @pl.when(row == 0)
            def _():
                b_local(k, k).start()

            @pl.when(row == 1)
            def _():
                b_recv_start(k)
        else:
            b_local(k, k).start()
        l_start(k, k)
    if off:
        for k in range(nb):
            @pl.when(row == 1)
            def _():
                b_local(k, nb + k).start()
    for t in range(nb, NBUF - 1):
        l_start(t, t)
    if not off:
        kept = lax.bitwise_xor((half - KEEP) // depth, col)
        for i, ref in enumerate((l0, l1, l2, l3)):
            @pl.when((row == 1) & (kept == i))
            def _():
                keep_copy(ref).start()

    def step(t, _):
        slot = lax.rem(t, NBUF)
        r, at = field(t, 0), field(t, 5)

        @pl.when(t + NBUF - 1 < n)
        def _():
            l_start(t + NBUF - 1, lax.rem(t + NBUF - 1, NBUF))

        @pl.when(field(t, 4) == 1)
        def _():
            b_local(0, at).wait()

        pltpu.make_async_copy(l0.at[pl.ds(0, TM), pl.ds(0, KB)], lv.at[slot], lsem.at[slot]).wait()
        rows_k = pl.ds(pl.multiple_of(at * KB, KB), KB)
        first = field(t, 2)

        @pl.when(first == 1)
        def _():
            acc[...] = DOT(lv[slot], bv[rows_k, :])

        @pl.when(first == 0)
        def _():
            acc[...] += DOT(lv[slot], bv[rows_k, :])

        @pl.when(field(t, 3) == 1)
        def _():
            if off:
                oslot = lax.rem(r, 2)

                @pl.when(r >= 2)
                def _():
                    o_copy(r - 2, oslot).wait()

                ov[oslot] = acc[...].astype(ov.dtype)
                o_copy(r, oslot).start()
            else:
                out[pl.ds(pl.multiple_of(r * TM, TM), TM), :] = acc[...]

        return 0

    lax.fori_loop(0, n, step, 0)
    if off:
        last = half // TM
        o_copy(last - 2, (last - 2) % 2).wait()
        o_copy(last - 1, (last - 1) % 2).wait()
    else:
        @pl.when(row == 1)
        def _():
            keep_copy(l0).wait()


def first_kernel(b_loc, out, sem):
    copy = pltpu.make_async_copy(b_loc.at[pl.ds(0, out.shape[0]), pl.ds(0, out.shape[1])], out, sem)

    @pl.when(lax.axis_index('row') == 0)
    def _():
        copy.start()
        copy.wait()


def tail_kernel(half, depth, k0, kw, src0, dst0, width, final, early, part, piece, *rest):
    row, col = lax.axis_index('row'), lax.axis_index('col')
    tm = FINE if final else TM
    tiles = half // tm
    kept = k0 >= half - KEEP
    if final:
        keep, (out, ov, osem) = rest[0], rest[-3:]
    elif kept:
        keep, out = rest
    else:
        l_refs, (out, bv, lv, lsem, bsem) = rest[:4], rest[4:]
    which = lax.bitwise_xor(k0 // depth, col)

    def l_copy(ref, t):
        slot = lax.rem(t, 2)
        return pltpu.make_async_copy(
            ref.at[pl.ds(t * tm, tm), pl.ds(k0 % depth, kw)], lv.at[slot], lsem.at[slot])

    def l_start(t):
        for i, ref in enumerate(l_refs):
            @pl.when(which == i)
            def _():
                l_copy(ref, t).start()

    def o_copy(t, c=src0):
        return pltpu.make_async_copy(
            ov.at[t], out.at[pl.ds(t * tm, tm), pl.ds(dst0 + c, width)], osem.at[t])

    def put(t, rows, total):
        if final:
            ov[t] = total.astype(ov.dtype)
            o_copy(t).start()
        else:
            out[rows, pl.ds(src0, width)] = total

    @pl.when(row == 1)
    def _():
        if not kept:
            b_copy = pltpu.make_async_copy(piece, bv, bsem)
            b_copy.start()
            l_start(0)
            l_start(1)
            b_copy.wait()
        right = piece if kept else bv

        def add(t, _):
            rows = pl.ds(pl.multiple_of(t * tm, tm), tm)
            if kept:
                tile = keep[rows, pl.ds(k0 - (half - KEEP), kw)]
            else:
                l_copy(l_refs[0], t).wait()
                tile = lv[lax.rem(t, 2)]
            put(t, rows, part[rows, pl.ds(src0, width)] + DOT(tile, right[...]))
            if not kept:
                @pl.when(t + 2 < tiles)
                def _():
                    l_start(t + 2)
            return 0

        lax.fori_loop(0, tiles, add, 0, unroll=kept)

    if final:
        @pl.when(row == 1)
        def _():
            for t in range(tiles):
                o_copy(t).wait()

    if early:
        @pl.when(row == 0)
        def _():
            for c in range(0, part.shape[1], width):
                def move(t, _):
                    rows = pl.ds(pl.multiple_of(t * tm, tm), tm)
                    ov[t] = part[rows, pl.ds(c, width)].astype(ov.dtype)
                    o_copy(t, c).start()
                    return 0

                lax.fori_loop(0, tiles, move, 0)
                for t in range(tiles):
                    o_copy(t, c).wait()


def solution(mesh):
    block_spec = P(('batch', 'row'), 'col')
    x_swap = [(0, 2), (1, 3), (2, 0), (3, 1)]
    core_swap = [(0, 1), (1, 0), (2, 3), (3, 2)]
    n_first = len(FIRST) + 1
    hbm = pl.BlockSpec(memory_space=pltpu.HBM)
    vmem = pl.BlockSpec(memory_space=pltpu.VMEM)
    smem = pl.BlockSpec(memory_space=pltpu.SMEM)

    def in_hbm(array):
        return pltpu.with_memory_space_constraint(array, pltpu.HBM)

    def product(l_block, b_block):
        half, depth = l_block.shape
        dtype = b_block.dtype
        off_counts, off_tab = plan(half, True)
        diag_counts, diag_tab = plan(half, False)
        info = jnp.stack([lax.axis_index('row'), lax.axis_index('col')]).astype(jnp.int32)
        starts = np.cumsum((0,) + WIDTHS).tolist()
        tail0, tail_w = starts[-1], b_block.shape[1] - starts[-1]

        cuts0 = np.cumsum((0,) + FIRST).tolist()
        boxes = [(r, e - r, 0, WIDTHS[0]) for r, e in zip(cuts0, cuts0[1:] + [half])]
        boxes += [(0, half, c, w) for c, w in zip(starts[1:], WIDTHS[1:])]
        n_main = len(boxes)
        ends = np.cumsum(TAIL).tolist()
        boxes += [(e - h, h, tail0, tail_w) for e, h in zip(ends[:-1], TAIL)]
        n_early, c = len(boxes) - 1, tail0
        for w, ks in LAST:
            boxes += [(half - TAIL[-1] + e - h, h, c, w) for e, h in zip(np.cumsum(ks).tolist(), ks)]
            c += w
        recv, source = [], b_block

        def send(j, source):
            r, h, c, w = boxes[j]
            if j == 0:
                piece = pl.pallas_call(
                    first_kernel, out_shape=pltpu.VMEM((h, w), dtype), in_specs=[hbm], out_specs=vmem,
                    scratch_shapes=[pltpu.SemaphoreType.DMA],
                    compiler_params=pltpu.CompilerParams(vmem_limit_bytes=2**20), name="first",
                )(in_hbm(source))
            else:
                piece = source[r:r + h, c:c + w]
            piece, source = lax.optimization_barrier((piece, source))
            recv.append(lax.ppermute(piece, 'row', [(0, 1), (1, 0)] if j == 0 else [(0, 1)]))
            return source

        for j in range(n_early):
            source = send(j, source)
        lx = lax.ppermute(l_block, 'col', x_swap)
        lc = lax.ppermute(l_block, 'col', core_swap)
        lxc = lax.ppermute(lx, 'col', core_swap)
        l_refs = [l_block, lc, lx, lxc]

        def chunk(pieces, cuts, x, src0, dst0, width, counts, tab):
            alias = [] if x is None else [x]
            operands = [tab, info, *map(in_hbm, [*l_refs, b_block, *pieces]), *alias]
            scratch = [
                pltpu.VMEM(((2 if cuts else 1) * half, width), dtype),
                pltpu.VMEM((NBUF, TM, KB), dtype),
                pltpu.VMEM((TM, width), jnp.float32),
            ]
            sems = [pltpu.SemaphoreType.DMA((NBUF,)), pltpu.SemaphoreType.DMA((2 * half // KB,))]
            if cuts:
                out, out_spec = jax.ShapeDtypeStruct(b_block.shape, dtype), hbm
                scratch += [pltpu.VMEM((2, TM, width), dtype), *sems, pltpu.SemaphoreType.DMA((2,))]
            else:
                out = (pltpu.VMEM((half, width), jnp.float32), pltpu.VMEM((half, KEEP), dtype))
                out_spec = (vmem, vmem)
                scratch += [*sems, pltpu.SemaphoreType.DMA]
            limit = 2 * (NBUF * TM * KB + (2 if cuts else 1) * half * width + 6 * TM * width) + 2 * 2**20
            return pl.pallas_call(
                functools.partial(chunk_kernel, half, depth, src0, dst0, width, counts, cuts, len(alias)),
                out_shape=out,
                in_specs=[smem, smem] + [hbm] * (len(operands) - 2), out_specs=out_spec,
                scratch_shapes=scratch,
                input_output_aliases={len(operands) - 1: 0} if alias else {},
                compiler_params=pltpu.CompilerParams(vmem_limit_bytes=limit),
                cost_estimate=pl.CostEstimate(flops=max(counts) * 2 * TM * KB * width,
                                              bytes_accessed=max(counts) * 2 * TM * KB, transcendentals=0),
            )(*operands)

        def tail(keep, piece, part, x, k0, kw, src0, width):
            final, kept = x is not None, k0 >= half - KEEP
            operands = [part, pltpu.with_memory_space_constraint(piece, pltpu.VMEM) if kept else in_hbm(piece)]
            operands += [keep] if kept else list(map(in_hbm, l_refs))
            specs = [vmem] + ([vmem, vmem] if kept else [hbm] * 5)
            scratch, need = [], 4 * TM * width + 2 * 2**20
            if final:
                operands.append(x)
                specs.append(hbm)
                out, out_spec = jax.ShapeDtypeStruct(x.shape, x.dtype), hbm
                scratch = [pltpu.VMEM((half // FINE, FINE, width), dtype), pltpu.SemaphoreType.DMA((half // FINE,))]
                need += 2 * half * width
            else:
                out, out_spec = pltpu.VMEM(part.shape, part.dtype), vmem
                if not kept:
                    scratch = [pltpu.VMEM((kw, width), dtype), pltpu.VMEM((2, TM, kw), dtype),
                               pltpu.SemaphoreType.DMA((2,)), pltpu.SemaphoreType.DMA]
                    need += 2 * kw * (width + 2 * TM)
            return pl.pallas_call(
                functools.partial(tail_kernel, half, depth, k0, kw, src0, tail0, width, final, final and src0 == 0),
                out_shape=out,
                in_specs=specs, out_specs=out_spec,
                scratch_shapes=scratch,
                input_output_aliases={len(operands) - 1: 0} if final else {0: 0},
                compiler_params=pltpu.CompilerParams(vmem_limit_bytes=need),
                cost_estimate=pl.CostEstimate(flops=2 * half * kw * width,
                                              bytes_accessed=2 * half * kw, transcendentals=0),
            )(*operands)

        x, part = None, None
        for j, width in enumerate(WIDTHS):
            if j == len(WIDTHS) - 1:
                x, b_block = lax.optimization_barrier((x, b_block))
                source = b_block
                for i in range(n_early, len(boxes)):
                    source = send(i, source)
                part, keep = chunk([], (), None, tail0, 0, tail_w, diag_counts, diag_tab)
                x, part, keep = lax.optimization_barrier((x, part, keep))
            pieces, cuts = (recv[:n_first], tuple(cuts0)) if j == 0 else ([recv[n_first - 1 + j]], (0,))
            x = chunk(pieces, cuts, x, starts[j], starts[j], width, off_counts, off_tab)
        x, part = lax.optimization_barrier((x, part))
        for piece, (k0, kw, c, w) in zip(recv[n_main:], boxes[n_main:]):
            final = k0 + kw == half
            done = tail(keep, piece, part, x if final else None, k0, kw, c - tail0, w)
            part, x = (part, done) if final else (done, x)
            x, part = lax.optimization_barrier((x, part))
        return x

    return jax.shard_map(product, mesh=mesh, in_specs=(block_spec, block_spec), out_specs=block_spec, check_vma=False)
```
